32 devices in a mesh: dom: 8 (over y, x, core), dim: 4 (over z).
Axes of the slice: x: 2, y: 2, z: 4, core: 2. Of those that a mesh axis runs over, the one named last changes fastest.
Arguments:
- particles: float32 [64, 1024], P('dom', 'dim'), may hold values from -5 to 5
- data_rows: bfloat16 [64, 16, 1024], P('dom', None, 'dim'), may hold values from -0.375 to 0.375
- labels: int32 [64, 16], P('dom'), may hold values from 0 to 1
Outputs:
- updates: float32 [2, 64, 1024], P(None, 'dom', 'dim')
The draws below stay inside these ranges and needn't reach their ends.
All inputs are finite; a program needn't handle non-finite values.
Results may differ from the reference program's by a relative error of at most 0.0003.
Values may be sent and summed in bfloat16 or wider, within the bound.
A program may use at most 64 MiB of HBM per device.

```python
import math
import jax
import jax.numpy as jnp
from jax import lax

D = 1024
R = 16
NEWTON = 2
CG_STEPS = 2
BAND = 1
PARTICLES = 64


def draw_particles(key, part):
    scale_key, value_key = jax.random.split(key, 2)
    spread = jnp.exp(jax.random.uniform(scale_key, (PARTICLES, 1), jnp.float32, math.log(0.4), math.log(1.1)))
    values = jax.random.truncated_normal(value_key, -4.0, 4.0, (PARTICLES, D), jnp.float32)
    return spread * values


def touch_ends(result, key, least, largest):
    shape = result.shape
    spot = [jax.random.randint(jax.random.fold_in(key, axis), (), 0, shape[axis]) for axis in range(len(shape))]
    result = result.at[tuple(spot)].set(least)
    longest = shape.index(max(shape))
    spot[longest] = (spot[longest] + 1) % shape[longest]
    return result.at[tuple(spot)].set(largest)


def shard_levels(rng, dims, shards, least, top_value):
    def one(axis_at, parts):
        heights = jax.random.uniform(jax.random.fold_in(jax.random.fold_in(rng, 6), axis_at), (parts,), jnp.float32, least / len(shards), top_value / len(shards))
        return jnp.repeat(jnp.exp(heights), dims[axis_at] // parts).reshape((-1,) + (1,) * (len(dims) - axis_at - 1))

    loudness = one(*shards[0])
    for cut in shards[1:]:
        loudness = loudness * one(*cut)
    return loudness


def noise(key, dims, width, limit, shards=(), kind=jnp.bfloat16):
    array = jax.random.normal(key, dims, jnp.float32) * width
    if len(shards) > 0:
        array = shard_levels(key, dims, shards, -0.22, 0.18) * array
    return jnp.clip(array, min=-limit, max=limit).astype(kind)


def setup_inputs(seed: int = 0) -> dict:
    keys = jax.random.split(jax.random.key(seed), 4)
    particles = draw_particles(jax.random.fold_in(keys[3], 71), 0)
    data_rows = noise(keys[1], (PARTICLES, R, D), (D // 4) ** -0.5, 0.375, ((0, 8), (2, 4)))
    labels = touch_ends(jax.random.randint(keys[2], (PARTICLES, R), 0, 2), jax.random.fold_in(keys[2], 1), 0, 1).astype(jnp.int32)
    return {"particles": particles, "data_rows": data_rows, "labels": labels}


prior_precision = 0.05
like_weight = 4.0
move_size = 0.5
highest = lax.Precision.HIGHEST


def reference(particles, data_rows, labels):
    factor_rows = data_rows.astype(jnp.float32)
    targets = labels.astype(jnp.float32)
    count = particles.shape[0]
    kernel_scale = 1.0 * BAND * D
    cross_scale = 4.0 / (kernel_scale * kernel_scale)
    current = particles
    outputs = []
    for newton_step in range(NEWTON):
        logits = jnp.einsum("jrd,jd->jr", factor_rows, current, precision=highest)
        probs = jax.nn.sigmoid(logits)
        gradient = -prior_precision * current + like_weight * jnp.einsum("jr,jrd->jd", targets - probs, factor_rows, precision=highest)
        curvature = like_weight * probs * (1.0 - probs)
        squares = jnp.sum(current * current, axis=1)
        inner_rows = jnp.dot(current, current.T, precision=highest)
        distance = squares[:, None] + squares[None, :] - 2.0 * inner_rows
        kernel = jnp.exp(-distance / kernel_scale)
        kernel_sq = kernel * kernel
        kernel_total = jnp.sum(kernel, axis=1)
        square_total = jnp.sum(kernel_sq, axis=1)
        kernel_grad = jnp.dot(kernel, gradient, precision=highest)
        kernel_pos = jnp.dot(kernel, current, precision=highest)
        square_pos = jnp.dot(kernel_sq, current, precision=highest)
        drift = (kernel_grad + (2.0 / kernel_scale) * (current * kernel_total[:, None] - kernel_pos)) / count

        def apply_operator(vectors):
            along_self = jnp.sum(current * vectors, axis=1)
            along_mean = jnp.sum(vectors * square_pos, axis=1)
            projected = jnp.einsum("jrd,id->jri", factor_rows, vectors, precision=highest)
            weighted = projected * curvature[:, :, None] * kernel_sq.T[:, None, :]
            pairs = jnp.einsum("jrd,jri->id", factor_rows, weighted, precision=highest)
            along_pair = jnp.dot(current, vectors.T, precision=highest)
            pairs = pairs + cross_scale * jnp.dot((kernel_sq.T * along_pair).T, current, precision=highest)
            local = prior_precision * square_total[:, None] * vectors + cross_scale * (current * (along_self * square_total - along_mean)[:, None] - along_self[:, None] * square_pos)
            return (pairs + local) / count

        solution = jnp.zeros_like(drift)
        residual = drift
        direction = drift
        norm_now = jnp.sum(residual * residual)
        for solve_step in range(CG_STEPS):
            image = apply_operator(direction)
            alpha = norm_now / jnp.sum(direction * image)
            solution = solution + alpha * direction
            residual = residual - alpha * image
            if solve_step + 1 < CG_STEPS:
                norm_next = jnp.sum(residual * residual)
                direction = residual + (norm_next / norm_now) * direction
                norm_now = norm_next
        outputs.append(solution)
        current = current + move_size * solution
    return jnp.stack(outputs)
```

```python
import functools

import jax
import jax.numpy as jnp
from jax import lax
from jax.experimental import pallas as pl
from jax.experimental.pallas import tpu as pltpu
from jax.sharding import PartitionSpec as P

NEWTON = 2
BAND = 1
LANES = 128

prior_precision = 0.05
like_weight = 4.0
move_size = 0.5
MESH = pl.DeviceIdType.MESH
f32 = jnp.float32
bf16 = jnp.bfloat16


def halves(v):
    high = v.astype(bf16).astype(f32)
    return jnp.concatenate([high, v - high], axis=0).astype(bf16)


def fold(product):
    rows = product.shape[0] // 2
    return product[:rows] + product[rows:]


def paired(product):
    half = product.shape[1] // 2
    return product[:, :half] + product[:, half:]


def dot(a, b):
    return lax.dot_general(a, b, (((1,), (0,)), ((), ())), preferred_element_type=f32)


def dot_t(a, b):
    return lax.dot_general(a, b, (((1,), (1,)), ((), ())), preferred_element_type=f32)


def total_of(values):
    return jnp.sum(jnp.sum(values, axis=0, keepdims=True), axis=1, keepdims=True)


def steps(
    nd, nz, x_ref, a_ref, y_ref, out_ref,
    rows_all, xbuf, xpieces, upd,
    x_recv, xd_recv, a_recv, ad_recv, send,
):
    rows, width = x_ref.shape
    draws = a_ref.shape[0]
    per_row = draws // rows
    chips = nd // 2
    count = nd * rows
    cols = nd * draws
    scale = 1.0 * BAND * width * nz
    cross = 4.0 / (scale * scale)
    me_dom = lax.axis_index("dom")
    z = lax.axis_index("dim")
    chip, core = me_dom // 2, me_dom % 2
    relay = chips == 4

    if relay:
        near = [chip + 1 - 2 * (chip % 2), chip + 2 - 4 * (chip // 2), 3 - chip]
    else:
        near = [(chip + m) % chips for m in range(1, chips)]
    if nz == 4:
        high = z // 2
        zs = [z + 1 - 2 * (z % 2), 2 - high, 3 - 3 * high]
    else:
        zs = [(z + k) % nz for k in range(1, nz)]
    planes = [z] + zs

    sent = []

    def copy(src, dst, recv, device):
        one = pltpu.make_async_remote_copy(
            src_ref=src, dst_ref=dst, send_sem=send.at[len(sent)], recv_sem=recv,
            device_id=device, device_id_type=MESH,
        )
        one.start()
        sent.append(one)

    def wait(dst, recv):
        pltpu.make_async_remote_copy(
            src_ref=dst, dst_ref=dst, send_sem=send.at[0], recv_sem=recv,
            device_id={"dom": me_dom + 1 - 2 * core}, device_id_type=MESH,
        ).wait_recv()

    def on_chip(c):
        return {"dom": c * 2 + core}

    partner = {"dom": me_dom + 1 - 2 * core}

    def xs(plane, c):
        return xbuf.at[plane, core, c]

    def whole(plane, c):
        return rows_all.at[plane, core, c]

    def part(plane, c, h):
        return rows_all.at[plane, core, c, pl.ds(h * (draws // 2), draws // 2)]

    barrier = pltpu.get_barrier_semaphore()
    greet = [on_chip(c) for c in near] + [{"dim": k} for k in zs] + [partner]
    for device in greet:
        pl.semaphore_signal(barrier, inc=1, device_id=device, device_id_type=MESH)

    lane_of = lax.broadcasted_iota(jnp.int32, (rows, draws), 1) // per_row
    row_of = lax.broadcasted_iota(jnp.int32, (rows, draws), 0)
    own_block = lane_of == row_of

    def flat(values):
        return jnp.sum(jnp.where(own_block, values, 0.0), axis=0, keepdims=True)

    tile = lax.broadcasted_iota(jnp.int32, (per_row, draws), 1) % per_row
    tile = (tile == lax.broadcasted_iota(jnp.int32, (per_row, draws), 0)).astype(f32).astype(bf16)
    labels = flat(dot(y_ref[...].astype(f32).astype(bf16), tile))
    own_x = x_ref[...]
    first = flat(fold(dot_t(halves(own_x), a_ref[...])))
    xbuf[z, core, chip, :, 0:width] = own_x
    xbuf[z, core, chip, :, width:] = jnp.concatenate([first, labels, jnp.zeros((rows - 2, draws), f32)], axis=0)
    rows_all[z, core, chip] = a_ref[...]
    pl.semaphore_wait(barrier, len(greet))

    for k in zs:
        copy(xs(z, chip), xs(z, chip), x_recv.at[z, chip], {"dim": k})
    for c in near:
        copy(xs(z, chip), xs(z, chip), x_recv.at[z, chip], on_chip(c))
    reach = near[:2] if relay else near
    for c in reach:
        copy(a_ref, whole(z, chip), a_recv.at[z, chip, 0], on_chip(c))
    for k in zs:
        copy(a_ref, whole(z, chip), a_recv.at[z, chip, 0], {"dim": k})

    def x_forward(plane):
        wait(xs(plane, chip), x_recv.at[plane, chip])
        for c in near:
            copy(xs(plane, chip), xs(plane, chip), x_recv.at[plane, chip], on_chip(c))

    def x_across(plane):
        for c in near:
            wait(xs(plane, c), x_recv.at[plane, c])
        copy(xbuf.at[plane, core], xbuf.at[plane, core], xd_recv.at[plane], partner)

    def a_forward(plane):
        wait(whole(plane, chip), a_recv.at[plane, chip, 0])
        for c in reach:
            copy(whole(plane, chip), whole(plane, chip), a_recv.at[plane, chip, 0], on_chip(c))

    def a_relay(plane):
        for m, c in enumerate(reach):
            wait(whole(plane, c), a_recv.at[plane, c, 0])
            if relay:
                copy(part(plane, c, m), part(plane, c, m), a_recv.at[plane, c, m], on_chip(near[1 - m]))

    def a_across(plane):
        if relay:
            for h in range(2):
                wait(part(plane, near[2], h), a_recv.at[plane, near[2], h])
        copy(rows_all.at[plane, core], rows_all.at[plane, core], ad_recv.at[plane], partner)

    for plane in zs:
        x_forward(plane)
    a_relay(z)
    x_across(z)
    for n, plane in enumerate(zs):
        a_forward(plane)
        if n == 0:
            x_across(plane)
            a_across(z)
        else:
            a_relay(zs[n - 1])
            x_across(plane)
            a_across(zs[n - 1])
    if nz > 1:
        a_relay(zs[-1])
        a_across(zs[-1])

    for plane in planes:
        wait(xbuf.at[plane, 1 - core], xd_recv.at[plane])
    eye = lax.broadcasted_iota(jnp.int32, (count, count), 1) == lax.broadcasted_iota(jnp.int32, (count, count), 0)
    for k in range(nz):
        upd[2, k] = xbuf[k, :, :, :, 0:width].reshape(count, width)

    def piece_x():
        for k in range(nz):
            xpieces[:, k * width : (k + 1) * width] = halves(upd[2, k])

    def row_sums(values):
        return jnp.sum(values, axis=1, keepdims=True)

    marks = functools.reduce(jnp.add, [xbuf[k, :, :, :, width:].reshape(count, draws) for k in range(nz)])
    targets = xbuf[0, :, :, :, width:].reshape(count, draws)
    logits = jnp.concatenate([marks[g * rows : g * rows + 1] for g in range(nd)], axis=0)
    targets = jnp.concatenate([targets[g * rows + 1 : g * rows + 2] for g in range(nd)], axis=0)
    spread_at = lax.broadcasted_iota(jnp.int32, (count, LANES), 1) // per_row
    for plane in planes:
        wait(rows_all.at[plane, 1 - core], ad_recv.at[plane])

    def back(on_rows, on_x):
        left = halves(on_rows)
        left_x = halves(jnp.concatenate([on_x, on_x], axis=1))
        parts = []
        for k in range(nz):
            product = dot(left, rows_all[k].reshape(cols, width))
            product = product + dot(left_x, xpieces[:, k * width : (k + 1) * width])
            parts.append(fold(product))
        return parts

    def ahead(parts):
        pieces = [halves(v) for v in parts]
        seen = functools.reduce(jnp.add, [dot_t(pieces[k], rows_all[k].reshape(cols, width)) for k in range(nz)])
        along = functools.reduce(
            jnp.add, [dot_t(pieces[k], xpieces[:, k * width : (k + 1) * width]) for k in range(nz)]
        )
        return fold(seen), paired(fold(along))

    def own_logits(seen):
        return jnp.concatenate(
            [flat(seen[g * rows : (g + 1) * rows, g * draws : (g + 1) * draws]) for g in range(nd)], axis=0
        )

    for t in range(NEWTON):
        last = t + 1 == NEWTON
        piece_x()
        inner = paired(fold(dot_t(xpieces[...], xpieces[...])))
        diagonal = jnp.where(eye, inner, 0.0)
        distance = row_sums(diagonal) + jnp.sum(diagonal, axis=0, keepdims=True) - 2.0 * inner
        kernel = jnp.exp(distance * (-1.0 / scale))
        prob = 1.0 / (1.0 + jnp.exp(-logits))
        curve = like_weight * prob * (1.0 - prob)
        gap = like_weight * (targets - prob)
        kernel_sq = kernel * kernel
        total = row_sums(kernel)
        total_sq = row_sums(kernel_sq)
        padded = kernel
        if count < LANES:
            padded = jnp.concatenate([kernel, jnp.zeros((count, LANES - count), f32)], axis=1)
        drive, weight = [], []
        for g in range(nd):
            at = g * rows
            block = padded[:, at // LANES * LANES : at // LANES * LANES + LANES]
            wide = jnp.take_along_axis(block, spread_at + at % LANES, axis=1)
            drive.append(wide * gap[g : g + 1])
            weight.append(wide * wide * curve[g : g + 1])
        drive = jnp.concatenate(drive, axis=1)
        weight = jnp.concatenate(weight, axis=1)
        pull = (-prior_precision - 2.0 / scale) * kernel + jnp.where(eye, (2.0 / scale) * total, 0.0)
        drift = [v / count for v in back(drive, pull)]
        seen, along = ahead(drift)
        shift = own_logits(seen)
        on_x = cross * kernel_sq * (along - row_sums(jnp.where(eye, along, 0.0)))
        on_x = on_x - jnp.where(eye, row_sums(on_x), 0.0)
        image = back(weight * seen, on_x)
        image = [(v + prior_precision * total_sq * d) / count for v, d in zip(image, drift)]
        seen, along = ahead(image)
        shift_image = own_logits(seen)
        along = along - row_sums(jnp.where(eye, along, 0.0))
        norm = total_of(functools.reduce(jnp.add, [d * d for d in drift]))
        curve_total = total_of(functools.reduce(jnp.add, [d * v for d, v in zip(drift, image)]))
        squares = functools.reduce(jnp.add, [v * v for v in image])
        image_square = total_of(squares)
        bent = total_of(prior_precision * total_sq * row_sums(squares) + cross * row_sums(kernel_sq * along * along))
        bent = (bent + total_of(weight * seen * seen)) / count
        alpha = norm / curve_total
        norm_next = norm - 2.0 * alpha * curve_total + alpha * alpha * image_square
        keep = 1.0 + norm_next / norm
        curve_next = keep * keep * curve_total - 2.0 * keep * alpha * image_square + alpha * alpha * bent
        alpha_next = norm_next / curve_next
        on_drift, on_image = alpha + alpha_next * keep, -alpha_next * alpha
        for k in range(nz):
            update = on_drift * drift[k] + on_image * image[k]
            upd[t, k] = update
            if not last:
                upd[2, k] = upd[2, k] + move_size * update
        if not last:
            logits = logits + move_size * (on_drift * shift + on_image * shift_image)
        out_ref[t] = upd[t, z, pl.ds(pl.multiple_of((core * chips + chip) * rows, rows), rows), :]
    for one in sent:
        one.wait_send()


def solution(mesh):
    nd, nz = mesh.shape["dom"], mesh.shape["dim"]

    def per_device(particles, data_rows, labels):
        rows, width = particles.shape
        draws = data_rows.shape[0] * data_rows.shape[1]
        count = nd * rows
        chips = nd // 2
        reach = 2 if chips == 4 else chips - 1
        number = (chips - 1 + nz - 1) + (reach + nz - 1) + (nz - 1) * (chips - 1 + reach) + 2 * nz
        if chips == 4:
            number += 2 * nz
        dma = pltpu.SemaphoreType.DMA
        return pl.pallas_call(
            functools.partial(steps, nd, nz),
            out_shape=jax.ShapeDtypeStruct((NEWTON, rows, width), f32),
            in_specs=[pl.BlockSpec(memory_space=pltpu.VMEM)] * 3,
            out_specs=pl.BlockSpec(memory_space=pltpu.VMEM),
            scratch_shapes=[
                pltpu.VMEM((nz, 2, chips, draws, width), bf16),
                pltpu.VMEM((nz, 2, chips, rows, width + draws), f32),
                pltpu.VMEM((2 * count, nz * width), bf16),
                pltpu.VMEM((NEWTON + 1, nz, count, width), f32),
                dma((nz, chips)),
                dma((nz,)),
                dma((nz, chips, 2)),
                dma((nz,)),
                dma((number,)),
            ],
            compiler_params=pltpu.CompilerParams(collective_id=0, has_side_effects=True),
        )(particles, data_rows.reshape(draws, width), labels)

    placed = (P("dom", "dim"), P("dom", None, "dim"), P("dom", None))
    return jax.shard_map(
        per_device, mesh=mesh, in_specs=placed, out_specs=P(None, "dom", "dim"), check_vma=False
    )
```

```python
import functools

import jax
import jax.numpy as jnp
from jax import lax
from jax.experimental import pallas as pl
from jax.experimental.pallas import tpu as pltpu
from jax.sharding import PartitionSpec as P

NEWTON = 2
BAND = 1
LANES = 128

prior_precision = 0.05
like_weight = 4.0
move_size = 0.5
MESH = pl.DeviceIdType.MESH
f32 = jnp.float32
bf16 = jnp.bfloat16


def halves(v):
    high = v.astype(bf16).astype(f32)
    return jnp.concatenate([high, v - high], axis=0).astype(bf16)


def fold(product):
    rows = product.shape[0] // 2
    return product[:rows] + product[rows:]


def paired(product):
    half = product.shape[1] // 2
    return product[:, :half] + product[:, half:]


def dot(a, b):
    return lax.dot_general(a, b, (((1,), (0,)), ((), ())), preferred_element_type=f32)


def dot_t(a, b):
    return lax.dot_general(a, b, (((1,), (1,)), ((), ())), preferred_element_type=f32)


def total_of(values):
    return jnp.sum(jnp.sum(values, axis=0, keepdims=True), axis=1, keepdims=True)


def steps(
    nd, nz, x_ref, a_ref, y_ref, out_ref,
    rows_all, xbuf, xpieces, upd,
    x_recv, x_over, a_recv, a_over, send,
):
    rows, width = x_ref.shape
    draws = a_ref.shape[0]
    per_row = draws // rows
    chips = nd // 2
    slots = nz * nd
    count = nd * rows
    cols = nd * draws
    scale = 1.0 * BAND * width * nz
    cross = 4.0 / (scale * scale)
    me_dom = lax.axis_index("dom")
    z = lax.axis_index("dim")
    chip, core = me_dom // 2, me_dom % 2
    square = chips == 4 and nz == 4

    if square:
        near = [chip + 1 - 2 * (chip % 2), chip + 2 - 4 * (chip // 2), 3 - chip]
        high = z // 2
        middle = (z + 1) // 2 % 2 == 1
        zs = [3 - 3 * high, 2 - high, z + 1 - 2 * (z % 2)]
    else:
        near = [(chip + m) % chips for m in range(1, chips)]
        zs = [(z + k) % nz for k in range(1, nz)]
    partner = {"dom": me_dom + 1 - 2 * core}
    started = {"x": 0, "a": 0, "p": 0}
    sems = {"x": send.at[0], "a": send.at[1], "p": send.at[2], "m": send.at[3]}

    def on_chip(c):
        return {"dom": c * 2 + core}

    def slot(plane, c, k=None):
        return (plane * 2 + (core if k is None else k)) * chips + c

    def copy(kind, ref, recv, device, src=None):
        pltpu.make_async_remote_copy(
            src_ref=ref if src is None else src, dst_ref=ref, send_sem=sems[kind], recv_sem=recv,
            device_id=device, device_id_type=MESH,
        ).start()
        if kind in started:
            started[kind] += 1

    def wait(ref, recv):
        pltpu.make_async_remote_copy(
            src_ref=ref, dst_ref=ref, send_sem=send.at[0], recv_sem=recv, device_id=partner, device_id_type=MESH,
        ).wait_recv()

    def wait_sent(ref, kind, number):
        while number > 0:
            part = ref.at[pl.ds(0, min(number, slots))]
            pltpu.make_async_remote_copy(
                src_ref=part, dst_ref=part, send_sem=sems[kind], recv_sem=send.at[0],
                device_id=partner, device_id_type=MESH,
            ).wait_send()
            number -= slots

    barrier = pltpu.get_barrier_semaphore()
    greet = [on_chip(c) for c in near] + [{"dim": k} for k in zs] + [partner]
    for device in greet:
        pl.semaphore_signal(barrier, inc=1, device_id=device, device_id_type=MESH)

    lane_of = lax.broadcasted_iota(jnp.int32, (rows, draws), 1) // per_row
    row_of = lax.broadcasted_iota(jnp.int32, (rows, draws), 0)
    own_block = lane_of == row_of

    def flat(values):
        return jnp.sum(jnp.where(own_block, values, 0.0), axis=0, keepdims=True)

    tile = lax.broadcasted_iota(jnp.int32, (per_row, draws), 1) % per_row
    tile = (tile == lax.broadcasted_iota(jnp.int32, (per_row, draws), 0)).astype(f32).astype(bf16)
    labels = flat(dot(y_ref[...].astype(f32).astype(bf16), tile))
    own_x = x_ref[...]
    first = flat(fold(dot_t(halves(own_x), a_ref[...])))
    here = slot(z, chip)
    xbuf[here, :, 0:width] = own_x
    xbuf[here, :, width:] = jnp.concatenate([first, labels, jnp.zeros((rows - 2, draws), f32)], axis=0)
    rows_all[here] = a_ref[...]
    pl.semaphore_wait(barrier, len(greet))

    def send_x(plane, devices, role):
        for device in devices:
            copy("x", xbuf.at[slot(plane, chip)], x_recv.at[plane, role], device)

    def send_a(plane, devices, role, src=None):
        for device in devices:
            copy("a", rows_all.at[slot(plane, chip)], a_recv.at[plane, role], device, src)

    plane_devices = [on_chip(c) for c in near]
    z_devices = [{"dim": k} for k in zs]
    side, diagonal = (near[:2], near[2]) if square else (near, None)
    send_x(z, z_devices, 0)
    send_x(z, plane_devices, 1)
    send_a(z, plane_devices[: len(side)], 1, a_ref)
    if square:
        send_a(z, plane_devices[2:], 2, a_ref)
    send_a(z, z_devices, 0, a_ref)
    for plane in zs:
        wait(xbuf.at[slot(plane, chip)], x_recv.at[plane, 0])
        send_x(plane, plane_devices, 1)

    def across(plane, c):
        copy("p", rows_all.at[slot(plane, c)], a_over.at[plane], partner)

    for n, plane in enumerate(zs):
        wait(rows_all.at[slot(plane, chip)], a_recv.at[plane, 0])
        if square and n == 0:
            send_a(plane, plane_devices[2:], 2)
        send_a(plane, plane_devices[: len(side)], 1)
        if square and n == 0:
            from_corner = rows_all.at[slot(z, diagonal)]
            wait(from_corner, a_recv.at[z, 2])
            copy("a", from_corner, a_recv.at[z, 2], z_devices[2])

            @pl.when(middle)
            def _():
                for device in z_devices[:2]:
                    copy("m", from_corner, a_recv.at[z, 2], device)

    for plane in [z] + zs:
        wait(xbuf.at[pl.ds(0, len(near))], x_recv.at[plane, 1])
        bundle = xbuf.at[pl.ds(slot(plane, 0), chips)]
        pltpu.make_async_remote_copy(
            src_ref=bundle, dst_ref=bundle, send_sem=sems["x"], recv_sem=x_over.at[plane],
            device_id=partner, device_id_type=MESH,
        ).start()
        started["x"] += chips

    across(z, chip)
    wait(rows_all.at[pl.ds(0, len(side))], a_recv.at[z, 1])
    for c in near:
        across(z, c)
    for plane in zs:
        across(plane, chip)
    for n, plane in enumerate(zs):
        if square and n == 0:
            wait(rows_all.at[slot(plane, diagonal)], a_recv.at[plane, 2])
            across(plane, diagonal)
        wait(rows_all.at[pl.ds(0, len(side))], a_recv.at[plane, 1])
        for c in side:
            across(plane, c)
    if square:
        for plane in zs[:0:-1]:
            wait(rows_all.at[slot(plane, diagonal)], a_recv.at[plane, 2])
            across(plane, diagonal)
    planes = [z] + zs
    for plane in planes:
        wait(xbuf.at[pl.ds(slot(plane, 0, 1 - core), chips)], x_over.at[plane])
    eye = lax.broadcasted_iota(jnp.int32, (count, count), 1) == lax.broadcasted_iota(jnp.int32, (count, count), 0)
    for k in range(nz):
        upd[2, k] = xbuf[k * nd : (k + 1) * nd, :, 0:width].reshape(count, width)

    def piece_x():
        for k in range(nz):
            xpieces[:, k * width : (k + 1) * width] = halves(upd[2, k])

    def row_sums(values):
        return jnp.sum(values, axis=1, keepdims=True)

    marks = functools.reduce(jnp.add, [xbuf[k * nd : (k + 1) * nd, :, width:].reshape(count, draws) for k in range(nz)])
    targets = xbuf[0:nd, :, width:].reshape(count, draws)
    logits = jnp.concatenate([marks[g * rows : g * rows + 1] for g in range(nd)], axis=0)
    targets = jnp.concatenate([targets[g * rows + 1 : g * rows + 2] for g in range(nd)], axis=0)
    spread_at = lax.broadcasted_iota(jnp.int32, (count, LANES), 1) // per_row
    for plane in planes:
        wait(rows_all.at[pl.ds(slot(plane, 0, 1 - core), chips)], a_over.at[plane])

    def basis(k):
        return rows_all[k * nd : (k + 1) * nd].reshape(cols, width)

    def back(on_rows, on_x):
        left = halves(on_rows)
        left_x = halves(jnp.concatenate([on_x, on_x], axis=1))
        parts = []
        for k in range(nz):
            product = dot(left, basis(k))
            product = product + dot(left_x, xpieces[:, k * width : (k + 1) * width])
            parts.append(fold(product))
        return parts

    def ahead(parts):
        pieces = [halves(v) for v in parts]
        seen = functools.reduce(jnp.add, [dot_t(pieces[k], basis(k)) for k in range(nz)])
        along = functools.reduce(
            jnp.add, [dot_t(pieces[k], xpieces[:, k * width : (k + 1) * width]) for k in range(nz)]
        )
        return fold(seen), paired(fold(along))

    def own_logits(seen):
        return jnp.concatenate(
            [flat(seen[g * rows : (g + 1) * rows, g * draws : (g + 1) * draws]) for g in range(nd)], axis=0
        )

    for t in range(NEWTON):
        last = t + 1 == NEWTON
        piece_x()
        inner = paired(fold(dot_t(xpieces[...], xpieces[...])))
        diagonal = jnp.where(eye, inner, 0.0)
        distance = row_sums(diagonal) + jnp.sum(diagonal, axis=0, keepdims=True) - 2.0 * inner
        kernel = jnp.exp(distance * (-1.0 / scale))
        prob = 1.0 / (1.0 + jnp.exp(-logits))
        curve = like_weight * prob * (1.0 - prob)
        gap = like_weight * (targets - prob)
        kernel_sq = kernel * kernel
        total = row_sums(kernel)
        total_sq = row_sums(kernel_sq)
        padded = kernel
        if count < LANES:
            padded = jnp.concatenate([kernel, jnp.zeros((count, LANES - count), f32)], axis=1)
        drive, weight = [], []
        for g in range(nd):
            at = g * rows
            block = padded[:, at // LANES * LANES : at // LANES * LANES + LANES]
            wide = jnp.take_along_axis(block, spread_at + at % LANES, axis=1)
            drive.append(wide * gap[g : g + 1])
            weight.append(wide * wide * curve[g : g + 1])
        drive = jnp.concatenate(drive, axis=1)
        weight = jnp.concatenate(weight, axis=1)
        pull = (-prior_precision - 2.0 / scale) * kernel + jnp.where(eye, (2.0 / scale) * total, 0.0)
        drift = [v / count for v in back(drive, pull)]
        seen, along = ahead(drift)
        shift = own_logits(seen)
        on_x = cross * kernel_sq * (along - row_sums(jnp.where(eye, along, 0.0)))
        on_x = on_x - jnp.where(eye, row_sums(on_x), 0.0)
        image = back(weight * seen, on_x)
        image = [(v + prior_precision * total_sq * d) / count for v, d in zip(image, drift)]
        seen, along = ahead(image)
        shift_image = own_logits(seen)
        along = along - row_sums(jnp.where(eye, along, 0.0))
        norm = total_of(functools.reduce(jnp.add, [d * d for d in drift]))
        curve_total = total_of(functools.reduce(jnp.add, [d * v for d, v in zip(drift, image)]))
        squares = functools.reduce(jnp.add, [v * v for v in image])
        image_square = total_of(squares)
        bent = total_of(prior_precision * total_sq * row_sums(squares) + cross * row_sums(kernel_sq * along * along))
        bent = (bent + total_of(weight * seen * seen)) / count
        alpha = norm / curve_total
        norm_next = norm - 2.0 * alpha * curve_total + alpha * alpha * image_square
        keep = 1.0 + norm_next / norm
        curve_next = keep * keep * curve_total - 2.0 * keep * alpha * image_square + alpha * alpha * bent
        alpha_next = norm_next / curve_next
        on_drift, on_image = alpha + alpha_next * keep, -alpha_next * alpha
        for k in range(nz):
            update = on_drift * drift[k] + on_image * image[k]
            upd[t, k] = update
            if not last:
                upd[2, k] = upd[2, k] + move_size * update
        if not last:
            logits = logits + move_size * (on_drift * shift + on_image * shift_image)
        out_ref[t] = upd[t, z, pl.ds(pl.multiple_of((core * chips + chip) * rows, rows), rows), :]
    wait_sent(xbuf, "x", started["x"])
    wait_sent(rows_all, "a", started["a"])
    wait_sent(rows_all, "p", started["p"])
    if square:

        @pl.when(middle)
        def _():
            wait_sent(rows_all, "m", 2)


def solution(mesh):
    nd, nz = mesh.shape["dom"], mesh.shape["dim"]

    def per_device(particles, data_rows, labels):
        rows, width = particles.shape
        draws = data_rows.shape[0] * data_rows.shape[1]
        count = nd * rows
        dma = pltpu.SemaphoreType.DMA
        return pl.pallas_call(
            functools.partial(steps, nd, nz),
            out_shape=jax.ShapeDtypeStruct((NEWTON, rows, width), f32),
            in_specs=[pl.BlockSpec(memory_space=pltpu.VMEM)] * 3,
            out_specs=pl.BlockSpec(memory_space=pltpu.VMEM),
            scratch_shapes=[
                pltpu.VMEM((nz * nd, draws, width), bf16),
                pltpu.VMEM((nz * nd, rows, width + draws), f32),
                pltpu.VMEM((2 * count, nz * width), bf16),
                pltpu.VMEM((NEWTON + 1, nz, count, width), f32),
                dma((nz, 2)),
                dma((nz,)),
                dma((nz, 3)),
                dma((nz,)),
                dma((4,)),
            ],
            compiler_params=pltpu.CompilerParams(collective_id=0, has_side_effects=True),
        )(particles, data_rows.reshape(draws, width), labels)

    placed = (P("dom", "dim"), P("dom", None, "dim"), P("dom", None))
    return jax.shard_map(
        per_device, mesh=mesh, in_specs=placed, out_specs=P(None, "dom", "dim"), check_vma=False
    )
```

```python
import functools

import jax
import jax.numpy as jnp
from jax import lax
from jax.experimental import pallas as pl
from jax.experimental.pallas import tpu as pltpu
from jax.sharding import PartitionSpec as P

NEWTON = 2
BAND = 1
LANES = 128

prior_precision = 0.05
like_weight = 4.0
move_size = 0.5
MESH = pl.DeviceIdType.MESH
f32 = jnp.float32
bf16 = jnp.bfloat16


def halves(v):
    high = v.astype(bf16).astype(f32)
    return jnp.concatenate([high, v - high], axis=0).astype(bf16)


def fold(product):
    rows = product.shape[0] // 2
    return product[:rows] + product[rows:]


def paired(product):
    half = product.shape[1] // 2
    return product[:, :half] + product[:, half:]


def dot(a, b):
    return lax.dot_general(a, b, (((1,), (0,)), ((), ())), preferred_element_type=f32)


def dot_t(a, b):
    return lax.dot_general(a, b, (((1,), (1,)), ((), ())), preferred_element_type=f32)


def total_of(values):
    return jnp.sum(jnp.sum(values, axis=0, keepdims=True), axis=1, keepdims=True)


def steps(
    nd, nz, x_ref, a_ref, y_ref, out_ref,
    rows_all, turned, xbuf, xpieces, place, firsts,
    signs, x_recv, x_over, a_recv, a_over, send, load,
):
    rows, width = x_ref.shape
    draws = a_ref.shape[0]
    per_row = draws // rows
    chips = nd // 2
    slots = nz * nd
    count = nd * rows
    cols = nd * draws
    scale = 1.0 * BAND * width * nz
    cross = 4.0 / (scale * scale)
    me_dom = lax.axis_index("dom")
    z = lax.axis_index("dim")
    chip, core = me_dom // 2, me_dom % 2
    square = chips == 4 and nz == 4

    if square:
        near = [chip + 1 - 2 * (chip % 2), chip + 2 - 4 * (chip // 2), 3 - chip]
        high = z // 2
        middle = (z + 1) // 2 % 2 == 1
        zs = [3 - 3 * high, 2 - high, z + 1 - 2 * (z % 2)]
    else:
        near = [(chip + m) % chips for m in range(1, chips)]
        zs = [(z + k) % nz for k in range(1, nz)]
    partner = {"dom": me_dom + 1 - 2 * core}
    started = {"x": 0, "a": 0, "p": 0}
    sems = {"x": send.at[0], "a": send.at[1], "p": send.at[2], "m": send.at[3]}

    def on_chip(c):
        return {"dom": c * 2 + core}

    def slot(plane, c, k=None):
        return (plane * 2 + (core if k is None else k)) * chips + c

    def copy(kind, ref, recv, device):
        pltpu.make_async_remote_copy(
            src_ref=ref, dst_ref=ref, send_sem=sems[kind], recv_sem=recv,
            device_id=device, device_id_type=MESH,
        ).start()
        if kind in started:
            started[kind] += 1

    def wait(ref, recv):
        pltpu.make_async_remote_copy(
            src_ref=ref, dst_ref=ref, send_sem=send.at[0], recv_sem=recv, device_id=partner, device_id_type=MESH,
        ).wait_recv()

    def wait_sent(ref, kind, number):
        while number > 0:
            part = ref.at[pl.ds(0, min(number, slots))]
            pltpu.make_async_remote_copy(
                src_ref=part, dst_ref=part, send_sem=sems[kind], recv_sem=send.at[0],
                device_id=partner, device_id_type=MESH,
            ).wait_send()
            number -= slots

    barrier = pltpu.get_barrier_semaphore()
    greet = [on_chip(c) for c in near] + [{"dim": k} for k in zs] + [partner]
    for device in greet:
        pl.semaphore_signal(barrier, inc=1, device_id=device, device_id_type=MESH)

    here = slot(z, chip)
    loads = [
        pltpu.make_async_copy(x_ref, xbuf.at[here, :, pl.ds(0, width)], load.at[0]),
        pltpu.make_async_copy(a_ref, rows_all.at[here], load.at[1]),
        pltpu.make_async_copy(y_ref, signs, load.at[2]),
    ]
    for one in loads:
        one.start()
    lane_of = lax.broadcasted_iota(jnp.int32, (rows, draws), 1) // per_row
    row_of = lax.broadcasted_iota(jnp.int32, (rows, draws), 0)
    own_block = lane_of == row_of

    def flat(values):
        return jnp.sum(jnp.where(own_block, values, 0.0), axis=0, keepdims=True)

    tile = lax.broadcasted_iota(jnp.int32, (per_row, draws), 1) % per_row
    tile = (tile == lax.broadcasted_iota(jnp.int32, (per_row, draws), 0)).astype(f32).astype(bf16)
    for one in loads:
        one.wait()
    labels = flat(dot(signs[...].astype(f32).astype(bf16), tile))
    first = flat(fold(dot_t(halves(xbuf[here, :, 0:width]), rows_all[here])))
    xbuf[here, :, width:] = jnp.concatenate([first, labels, jnp.zeros((rows - 2, draws), f32)], axis=0)
    pl.semaphore_wait(barrier, len(greet))

    def send_x(plane, devices, role):
        for device in devices:
            copy("x", xbuf.at[slot(plane, chip)], x_recv.at[plane, role], device)

    def send_a(plane, devices, role):
        for device in devices:
            copy("a", rows_all.at[slot(plane, chip)], a_recv.at[plane, role], device)

    plane_devices = [on_chip(c) for c in near]
    z_devices = [{"dim": k} for k in zs]
    side, diagonal = (near[:2], near[2]) if square else (near, None)
    send_x(z, z_devices, 0)
    send_x(z, plane_devices, 1)
    send_a(z, plane_devices[: len(side)], 1)
    if square:
        send_a(z, plane_devices[2:], 2)
    send_a(z, z_devices, 0)
    for plane in zs:
        wait(xbuf.at[slot(plane, chip)], x_recv.at[plane, 0])
        send_x(plane, plane_devices, 1)

    def across(plane, c):
        copy("p", rows_all.at[slot(plane, c)], a_over.at[plane], partner)

    for n, plane in enumerate(zs):
        wait(rows_all.at[slot(plane, chip)], a_recv.at[plane, 0])
        if square and n == 0:
            send_a(plane, plane_devices[2:], 2)
        send_a(plane, plane_devices[: len(side)], 1)
        if square and n == 0:
            from_corner = rows_all.at[slot(z, diagonal)]
            wait(from_corner, a_recv.at[z, 2])
            copy("a", from_corner, a_recv.at[z, 2], z_devices[2])

            @pl.when(middle)
            def _():
                for device in z_devices[:2]:
                    copy("m", from_corner, a_recv.at[z, 2], device)

    for plane in [z] + zs:
        wait(xbuf.at[pl.ds(0, len(near))], x_recv.at[plane, 1])
        bundle = xbuf.at[pl.ds(slot(plane, 0), chips)]
        pltpu.make_async_remote_copy(
            src_ref=bundle, dst_ref=bundle, send_sem=sems["x"], recv_sem=x_over.at[plane],
            device_id=partner, device_id_type=MESH,
        ).start()
        started["x"] += chips

    across(z, chip)
    wait(rows_all.at[pl.ds(0, len(side))], a_recv.at[z, 1])
    for c in near:
        across(z, c)
    for plane in zs:
        across(plane, chip)
    planes = [z] + zs
    for plane in planes:
        wait(xbuf.at[pl.ds(slot(plane, 0, 1 - core), chips)], x_over.at[plane])
    eye = lax.broadcasted_iota(jnp.int32, (count, count), 1) == lax.broadcasted_iota(jnp.int32, (count, count), 0)
    spread_at = lax.broadcasted_iota(jnp.int32, (count, LANES), 1) // per_row
    for k in range(nz):
        place[k] = xbuf[k * nd : (k + 1) * nd, :, 0:width].reshape(count, width)

    def row_sums(values):
        return jnp.sum(values, axis=1, keepdims=True)

    marks = functools.reduce(jnp.add, [xbuf[k * nd : (k + 1) * nd, :, width:].reshape(count, draws) for k in range(nz)])
    targets = xbuf[0:nd, :, width:].reshape(count, draws)
    logits = jnp.concatenate([marks[g * rows : g * rows + 1] for g in range(nd)], axis=0)
    targets = jnp.concatenate([targets[g * rows + 1 : g * rows + 2] for g in range(nd)], axis=0)

    def prepare(logits):
        for k in range(nz):
            xpieces[k] = halves(place[k])
        inner = paired(fold(functools.reduce(jnp.add, [dot_t(xpieces[k], xpieces[k]) for k in range(nz)])))
        diagonal = jnp.where(eye, inner, 0.0)
        distance = row_sums(diagonal) + jnp.sum(diagonal, axis=0, keepdims=True) - 2.0 * inner
        kernel = jnp.exp(distance * (-1.0 / scale))
        prob = 1.0 / (1.0 + jnp.exp(-logits))
        curve = like_weight * prob * (1.0 - prob)
        gap = like_weight * (targets - prob)
        kernel_sq = kernel * kernel
        padded = kernel
        if count < LANES:
            padded = jnp.concatenate([kernel, jnp.zeros((count, LANES - count), f32)], axis=1)
        drive, weight = [], []
        for g in range(nd):
            at = g * rows
            block = padded[:, at // LANES * LANES : at // LANES * LANES + LANES]
            wide = jnp.take_along_axis(block, spread_at + at % LANES, axis=1)
            drive.append(wide * gap[g : g + 1])
            weight.append(wide * wide * curve[g : g + 1])
        pull = (-prior_precision - 2.0 / scale) * kernel + jnp.where(eye, (2.0 / scale) * row_sums(kernel), 0.0)
        drive, weight = jnp.concatenate(drive, axis=1), jnp.concatenate(weight, axis=1)
        return kernel_sq, row_sums(kernel_sq), weight, drive, pull

    def basis(k):
        return rows_all[pl.ds(k * nd, nd)].reshape(cols, width)

    def lefts(on_rows, on_x):
        return halves(on_rows), halves(jnp.concatenate([on_x, on_x], axis=1))

    def back(left, left_x, k):
        return fold(dot(left, basis(k)) + dot(left_x, xpieces[k]))

    def ahead(parts):
        pieces = [halves(v) for v in parts]
        seen = dot(jnp.concatenate(pieces, axis=1), turned[...])
        along = functools.reduce(jnp.add, [dot_t(pieces[k], xpieces[k]) for k in range(nz)])
        return fold(seen), paired(fold(along))

    def own_logits(seen):
        return jnp.concatenate(
            [flat(seen[g * rows : (g + 1) * rows, g * draws : (g + 1) * draws]) for g in range(nd)], axis=0
        )

    kernel_sq, total_sq, weight, drive, pull = prepare(logits)
    left, left_x = lefts(drive, pull)

    def begin(plane):
        wait(rows_all.at[pl.ds(slot(plane, 0, 1 - core), chips)], a_over.at[plane])
        part = back(left, left_x, plane) / count
        firsts[plane] = part
        pieces = halves(part)
        turned[pl.ds(pl.multiple_of(plane * width, width), width), :] = basis(plane).T
        return dot_t(pieces, basis(plane)), dot_t(pieces, xpieces[plane])

    started_parts = [begin(z)]
    for n, plane in enumerate(zs):
        if square and n == 0:
            wait(rows_all.at[slot(plane, diagonal)], a_recv.at[plane, 2])
            across(plane, diagonal)
        wait(rows_all.at[pl.ds(0, len(side))], a_recv.at[plane, 1])
        for c in side:
            across(plane, c)
    if square:
        for plane in zs[:0:-1]:
            wait(rows_all.at[slot(plane, diagonal)], a_recv.at[plane, 2])
            across(plane, diagonal)
    started_parts += [begin(plane) for plane in zs]
    seen = fold(functools.reduce(jnp.add, [part[0] for part in started_parts]))
    along = paired(fold(functools.reduce(jnp.add, [part[1] for part in started_parts])))
    drift = [firsts[k] for k in range(nz)]

    for t in range(NEWTON):
        last = t + 1 == NEWTON
        if t > 0:
            kernel_sq, total_sq, weight, drive, pull = prepare(logits)
            left, left_x = lefts(drive, pull)
            drift = [back(left, left_x, k) / count for k in range(nz)]
            seen, along = ahead(drift)
        shift = own_logits(seen)
        on_x = cross * kernel_sq * (along - row_sums(jnp.where(eye, along, 0.0)))
        on_x = on_x - jnp.where(eye, row_sums(on_x), 0.0)
        left, left_x = lefts(weight * seen, on_x)
        image = [(back(left, left_x, k) + prior_precision * total_sq * drift[k]) / count for k in range(nz)]
        seen, along = ahead(image)
        shift_image = own_logits(seen)
        along = along - row_sums(jnp.where(eye, along, 0.0))
        norm = total_of(functools.reduce(jnp.add, [d * d for d in drift]))
        curve_total = total_of(functools.reduce(jnp.add, [d * v for d, v in zip(drift, image)]))
        squares = functools.reduce(jnp.add, [v * v for v in image])
        image_square = total_of(squares)
        bent = total_of(prior_precision * total_sq * row_sums(squares) + cross * row_sums(kernel_sq * along * along))
        bent = (bent + total_of(weight * seen * seen)) / count
        alpha = norm / curve_total
        norm_next = norm - 2.0 * alpha * curve_total + alpha * alpha * image_square
        keep = 1.0 + norm_next / norm
        curve_next = keep * keep * curve_total - 2.0 * keep * alpha * image_square + alpha * alpha * bent
        alpha_next = norm_next / curve_next
        on_drift, on_image = alpha + alpha_next * keep, -alpha_next * alpha
        for k in range(nz):
            firsts[k] = on_drift * drift[k] + on_image * image[k]
        out_ref[t] = firsts[z, pl.ds(pl.multiple_of((core * chips + chip) * rows, rows), rows), :]
        if not last:
            for k in range(nz):
                place[k] = place[k] + move_size * firsts[k]
            logits = logits + move_size * (on_drift * shift + on_image * shift_image)
    wait_sent(xbuf, "x", started["x"])
    wait_sent(rows_all, "a", started["a"])
    wait_sent(rows_all, "p", started["p"])
    if square:

        @pl.when(middle)
        def _():
            wait_sent(rows_all, "m", 2)


def solution(mesh):
    nd, nz = mesh.shape["dom"], mesh.shape["dim"]

    def per_device(particles, data_rows, labels):
        rows, width = particles.shape
        draws = data_rows.shape[0] * data_rows.shape[1]
        count = nd * rows
        dma = pltpu.SemaphoreType.DMA
        return pl.pallas_call(
            functools.partial(steps, nd, nz),
            out_shape=pltpu.VMEM((NEWTON, rows, width), f32),
            in_specs=[pl.BlockSpec(memory_space=pl.ANY)] * 3,
            out_specs=pl.BlockSpec(memory_space=pltpu.VMEM),
            scratch_shapes=[
                pltpu.VMEM((nz * nd, draws, width), bf16),
                pltpu.VMEM((nz * width, nd * draws), bf16),
                pltpu.VMEM((nz * nd, rows, width + draws), f32),
                pltpu.VMEM((nz, 2 * count, width), bf16),
                pltpu.VMEM((nz, count, width), f32),
                pltpu.VMEM((nz, count, width), f32),
                pltpu.VMEM(labels.shape, jnp.int32),
                dma((nz, 2)),
                dma((nz,)),
                dma((nz, 3)),
                dma((nz,)),
                dma((4,)),
                dma((3,)),
            ],
            compiler_params=pltpu.CompilerParams(collective_id=0, has_side_effects=True, vmem_limit_bytes=67_000_000),
        )(particles, data_rows.reshape(draws, width), labels)

    placed = (P("dom", "dim"), P("dom", None, "dim"), P("dom", None))
    return jax.shard_map(
        per_device, mesh=mesh, in_specs=placed, out_specs=P(None, "dom", "dim"), check_vma=False
    )
```

```python
import functools

import jax
import jax.numpy as jnp
from jax import lax
from jax.experimental import pallas as pl
from jax.experimental.pallas import tpu as pltpu
from jax.sharding import PartitionSpec as P

NEWTON = 2
BAND = 1
LANES = 128

prior_precision = 0.05
like_weight = 4.0
move_size = 0.5
MESH = pl.DeviceIdType.MESH
f32 = jnp.float32
bf16 = jnp.bfloat16


def halves(v):
    high = v.astype(bf16).astype(f32)
    return jnp.concatenate([high, v - high], axis=0).astype(bf16)


def fold(product):
    rows = product.shape[0] // 2
    return product[:rows] + product[rows:]


def paired(product):
    half = product.shape[1] // 2
    return product[:, :half] + product[:, half:]


def dot(a, b):
    return lax.dot_general(a, b, (((1,), (0,)), ((), ())), preferred_element_type=f32)


def dot_t(a, b):
    return lax.dot_general(a, b, (((1,), (1,)), ((), ())), preferred_element_type=f32)


def total_of(values):
    return jnp.sum(jnp.sum(values, axis=0, keepdims=True), axis=1, keepdims=True)


def steps(
    nd, nz, x_ref, a_ref, y_ref, out_ref,
    rows_all, turned, xbuf, xpieces, place, firsts,
    signs, x_recv, x_over, a_recv, a_over, send, load,
):
    rows, width = x_ref.shape
    draws = a_ref.shape[0]
    per_row = draws // rows
    chips = nd // 2
    slots = nz * nd
    count = nd * rows
    cols = nd * draws
    blocks = width // LANES
    message = blocks * rows + 2
    scale = 1.0 * BAND * width * nz
    cross = 4.0 / (scale * scale)
    me_dom = lax.axis_index("dom")
    z = lax.axis_index("dim")
    chip, core = me_dom // 2, me_dom % 2
    square = chips == 4 and nz == 4

    if square:
        near = [chip + 1 - 2 * (chip % 2), chip + 2 - 4 * (chip // 2), 3 - chip]
        high = z // 2
        middle = (z + 1) // 2 % 2 == 1
        zs = [3 - 3 * high, 2 - high, z + 1 - 2 * (z % 2)]
    else:
        near = [(chip + m) % chips for m in range(1, chips)]
        zs = [(z + k) % nz for k in range(1, nz)]
    partner = {"dom": me_dom + 1 - 2 * core}
    started = {"x": 0, "a": 0, "p": 0}
    sems = {"x": send.at[0], "a": send.at[1], "p": send.at[2], "m": send.at[3]}

    def on_chip(c):
        return {"dom": c * 2 + core}

    def slot(plane, c, k=None):
        return (plane * 2 + (core if k is None else k)) * chips + c

    def copy(kind, ref, recv, device):
        pltpu.make_async_remote_copy(
            src_ref=ref, dst_ref=ref, send_sem=sems[kind], recv_sem=recv,
            device_id=device, device_id_type=MESH,
        ).start()
        if kind in started:
            started[kind] += 1

    def wait(ref, recv):
        pltpu.make_async_remote_copy(
            src_ref=ref, dst_ref=ref, send_sem=send.at[0], recv_sem=recv, device_id=partner, device_id_type=MESH,
        ).wait_recv()

    def wait_sent(ref, kind, number):
        while number > 0:
            part = ref(min(number, slots))
            pltpu.make_async_remote_copy(
                src_ref=part, dst_ref=part, send_sem=sems[kind], recv_sem=send.at[0],
                device_id=partner, device_id_type=MESH,
            ).wait_send()
            number -= slots

    barrier = pltpu.get_barrier_semaphore()
    greet = [on_chip(c) for c in near] + [{"dim": k} for k in zs] + [partner]
    for device in greet:
        pl.semaphore_signal(barrier, inc=1, device_id=device, device_id_type=MESH)

    here = slot(z, chip)
    loads = [
        pltpu.make_async_copy(
            x_ref.at[:, pl.ds(b * LANES, LANES)], xbuf.at[here, pl.ds(b * rows, rows), :], load.at[2 + b]
        )
        for b in range(blocks)
    ]
    loads.append(pltpu.make_async_copy(a_ref, rows_all.at[here], load.at[0]))
    loads.append(pltpu.make_async_copy(y_ref, signs, load.at[1]))
    for one in loads:
        one.start()
    lane_of = lax.broadcasted_iota(jnp.int32, (rows, draws), 1) // per_row
    row_of = lax.broadcasted_iota(jnp.int32, (rows, draws), 0)
    own_block = lane_of == row_of

    def flat(values):
        return jnp.sum(jnp.where(own_block, values, 0.0), axis=0, keepdims=True)

    tile = lax.broadcasted_iota(jnp.int32, (per_row, draws), 1) % per_row
    tile = (tile == lax.broadcasted_iota(jnp.int32, (per_row, draws), 0)).astype(f32).astype(bf16)
    for one in loads:
        one.wait()
    labels = flat(dot(signs[...].astype(f32).astype(bf16), tile))
    own_x = jnp.concatenate([xbuf[here, b * rows : (b + 1) * rows, :] for b in range(blocks)], axis=1)
    first = flat(fold(dot_t(halves(own_x), rows_all[here])))
    xbuf[here, blocks * rows : blocks * rows + 2, :] = jnp.concatenate([first, labels], axis=0)
    pl.semaphore_wait(barrier, len(greet))

    def xs(at, number=None):
        return xbuf.at[at if number is None else pl.ds(at, number), pl.ds(0, message), :]

    def send_x(plane, devices, role):
        for device in devices:
            copy("x", xs(slot(plane, chip)), x_recv.at[plane, role], device)

    def send_a(plane, devices, role):
        for device in devices:
            copy("a", rows_all.at[slot(plane, chip)], a_recv.at[plane, role], device)

    plane_devices = [on_chip(c) for c in near]
    z_devices = [{"dim": k} for k in zs]
    side, diagonal = (near[:2], near[2]) if square else (near, None)
    send_x(z, z_devices, 0)
    send_x(z, plane_devices, 1)
    if square:
        send_a(z, plane_devices[2:], 2)
    send_a(z, plane_devices[: len(side)], 1)
    send_a(z, z_devices, 0)
    for plane in zs:
        wait(xs(slot(plane, chip)), x_recv.at[plane, 0])
        send_x(plane, plane_devices, 1)

    def across(plane, c):
        copy("p", rows_all.at[slot(plane, c)], a_over.at[plane], partner)

    for n, plane in enumerate(zs):
        wait(rows_all.at[slot(plane, chip)], a_recv.at[plane, 0])
        if square and n == 0:
            send_a(plane, plane_devices[2:], 2)
        send_a(plane, plane_devices[: len(side)], 1)
        if square and n == 0:
            from_corner = rows_all.at[slot(z, diagonal)]
            wait(from_corner, a_recv.at[z, 2])
            copy("a", from_corner, a_recv.at[z, 2], z_devices[2])

            @pl.when(middle)
            def _():
                for device in z_devices[:2]:
                    copy("m", from_corner, a_recv.at[z, 2], device)

    for plane in [z] + zs:
        wait(xs(0, len(near)), x_recv.at[plane, 1])
        bundle = xs(slot(plane, 0), chips)
        pltpu.make_async_remote_copy(
            src_ref=bundle, dst_ref=bundle, send_sem=sems["x"], recv_sem=x_over.at[plane],
            device_id=partner, device_id_type=MESH,
        ).start()
        started["x"] += chips

    across(z, chip)
    wait(rows_all.at[pl.ds(0, len(side))], a_recv.at[z, 1])
    for c in near:
        across(z, c)
    for plane in zs:
        across(plane, chip)
    eye = lax.broadcasted_iota(jnp.int32, (count, count), 1) == lax.broadcasted_iota(jnp.int32, (count, count), 0)
    spread_at = lax.broadcasted_iota(jnp.int32, (count, LANES), 1) // per_row
    def row_sums(values):
        return jnp.sum(values, axis=1, keepdims=True)

    def prepare(logits):
        for k in range(nz):
            xpieces[k] = halves(place[k])
        inner = paired(fold(functools.reduce(jnp.add, [dot_t(xpieces[k], xpieces[k]) for k in range(nz)])))
        diagonal = jnp.where(eye, inner, 0.0)
        distance = row_sums(diagonal) + jnp.sum(diagonal, axis=0, keepdims=True) - 2.0 * inner
        kernel = jnp.exp(distance * (-1.0 / scale))
        prob = 1.0 / (1.0 + jnp.exp(-logits))
        curve = like_weight * prob * (1.0 - prob)
        gap = like_weight * (targets - prob)
        kernel_sq = kernel * kernel
        padded = kernel
        if count < LANES:
            padded = jnp.concatenate([kernel, jnp.zeros((count, LANES - count), f32)], axis=1)
        drive, weight = [], []
        for g in range(nd):
            at = g * rows
            block = padded[:, at // LANES * LANES : at // LANES * LANES + LANES]
            wide = jnp.take_along_axis(block, spread_at + at % LANES, axis=1)
            drive.append(wide * gap[g : g + 1])
            weight.append(wide * wide * curve[g : g + 1])
        pull = (-prior_precision - 2.0 / scale) * kernel + jnp.where(eye, (2.0 / scale) * row_sums(kernel), 0.0)
        drive, weight = jnp.concatenate(drive, axis=1), jnp.concatenate(weight, axis=1)
        return kernel_sq, row_sums(kernel_sq), weight, drive, pull

    def basis(k):
        return rows_all[pl.ds(k * nd, nd)].reshape(cols, width)

    def ahead(parts):
        seen = dot(jnp.concatenate([halves(v) for v in parts], axis=1), turned[...])
        along = functools.reduce(jnp.add, [dot_t(parts[k].astype(bf16), xpieces[k, 0:count]) for k in range(nz)])
        return fold(seen), along

    def own_logits(seen):
        return jnp.concatenate(
            [flat(seen[g * rows : (g + 1) * rows, g * draws : (g + 1) * draws]) for g in range(nd)], axis=0
        )


    def hand_over(n):
        plane = zs[n]
        if square and n == 0:
            wait(rows_all.at[slot(plane, diagonal)], a_recv.at[plane, 2])
            across(plane, diagonal)
        wait(rows_all.at[pl.ds(0, len(side))], a_recv.at[plane, 1])
        for c in side:
            across(plane, c)

    def hand_corners():
        if square:
            for plane in zs[:0:-1]:
                wait(rows_all.at[slot(plane, diagonal)], a_recv.at[plane, 2])
                across(plane, diagonal)

    if len(zs) > 0:
        hand_over(0)
    planes = [z] + zs
    for plane in planes:
        wait(xs(slot(plane, 0, 1 - core), chips), x_over.at[plane])
    for k in range(nz):
        for b in range(blocks):
            block = xbuf[k * nd : (k + 1) * nd, b * rows : (b + 1) * rows, :].reshape(count, LANES)
            place[k, :, b * LANES : (b + 1) * LANES] = block

    def messages(k, row):
        return jnp.concatenate([xbuf[k * nd + g, row : row + 1, :] for g in range(nd)], axis=0)

    logits = functools.reduce(jnp.add, [messages(k, blocks * rows) for k in range(nz)])
    targets = messages(0, blocks * rows + 1)

    kernel_sq, total_sq, weight, drive, pull = prepare(logits)
    left = halves(drive)
    left_x = halves(jnp.concatenate([pull, pull], axis=1))

    def begin(plane):
        wait(rows_all.at[pl.ds(slot(plane, 0, 1 - core), chips)], a_over.at[plane])
        rows_here = basis(plane)
        part = fold(dot(left, rows_here) + dot(left_x, xpieces[plane])) / count
        firsts[plane] = part
        turned[pl.ds(pl.multiple_of(plane * width, width), width), :] = rows_here.T
        return dot_t(halves(part), rows_here), dot_t(part.astype(bf16), xpieces[plane, 0:count])

    started_parts = [begin(z)]
    if len(zs) > 1:
        hand_over(1)
    if len(zs) > 2:
        hand_over(2)
    hand_corners()
    started_parts += [begin(plane) for plane in zs]
    seen = fold(functools.reduce(jnp.add, [part[0] for part in started_parts]))
    along = functools.reduce(jnp.add, [part[1] for part in started_parts])
    drift = [firsts[k] for k in range(nz)]

    for t in range(NEWTON):
        last = t + 1 == NEWTON
        if t > 0:
            kernel_sq, total_sq, weight, drive, pull = prepare(logits)
            left = halves(drive)
            left_x = halves(jnp.concatenate([pull, pull], axis=1))
            drift = [fold(dot(left, basis(k)) + dot(left_x, xpieces[k])) / count for k in range(nz)]
            seen, along = ahead(drift)
        shift = own_logits(seen)
        on_x = cross * kernel_sq * (along - row_sums(jnp.where(eye, along, 0.0)))
        on_x = on_x - jnp.where(eye, row_sums(on_x), 0.0)
        left, left_x = halves(weight * seen), on_x.astype(bf16)
        image = [
            (fold(dot(left, basis(k))) + dot(left_x, xpieces[k, 0:count]) + prior_precision * total_sq * drift[k])
            / count
            for k in range(nz)
        ]
        seen, along = ahead(image)
        shift_image = own_logits(seen)
        along = along - row_sums(jnp.where(eye, along, 0.0))
        norm = total_of(functools.reduce(jnp.add, [d * d for d in drift]))
        curve_total = total_of(functools.reduce(jnp.add, [d * v for d, v in zip(drift, image)]))
        squares = functools.reduce(jnp.add, [v * v for v in image])
        image_square = total_of(squares)
        bent = total_of(prior_precision * total_sq * row_sums(squares) + cross * row_sums(kernel_sq * along * along))
        bent = (bent + total_of(weight * seen * seen)) / count
        alpha = norm / curve_total
        norm_next = norm - 2.0 * alpha * curve_total + alpha * alpha * image_square
        keep = 1.0 + norm_next / norm
        curve_next = keep * keep * curve_total - 2.0 * keep * alpha * image_square + alpha * alpha * bent
        alpha_next = norm_next / curve_next
        on_drift, on_image = alpha + alpha_next * keep, -alpha_next * alpha
        for k in range(nz):
            firsts[k] = on_drift * drift[k] + on_image * image[k]
        out_ref[t] = firsts[z, pl.ds(pl.multiple_of((core * chips + chip) * rows, rows), rows), :]
        if not last:
            for k in range(nz):
                place[k] = place[k] + move_size * firsts[k]
            logits = logits + move_size * (on_drift * shift + on_image * shift_image)
    wait_sent(lambda number: xs(0, number), "x", started["x"])
    wait_sent(lambda number: rows_all.at[pl.ds(0, number)], "a", started["a"])
    wait_sent(lambda number: rows_all.at[pl.ds(0, number)], "p", started["p"])
    if square:

        @pl.when(middle)
        def _():
            wait_sent(lambda number: rows_all.at[pl.ds(0, number)], "m", 2)


def solution(mesh):
    nd, nz = mesh.shape["dom"], mesh.shape["dim"]

    def per_device(particles, data_rows, labels):
        rows, width = particles.shape
        draws = data_rows.shape[0] * data_rows.shape[1]
        count = nd * rows
        dma = pltpu.SemaphoreType.DMA
        return pl.pallas_call(
            functools.partial(steps, nd, nz),
            out_shape=pltpu.VMEM((NEWTON, rows, width), f32),
            in_specs=[pl.BlockSpec(memory_space=pl.ANY)] * 3,
            out_specs=pl.BlockSpec(memory_space=pltpu.VMEM),
            scratch_shapes=[
                pltpu.VMEM((nz * nd, draws, width), bf16),
                pltpu.VMEM((nz * width, nd * draws), bf16),
                pltpu.VMEM((nz * nd, -(-(width // LANES * rows + 2) // 8) * 8, LANES), f32),
                pltpu.VMEM((nz, 2 * count, width), bf16),
                pltpu.VMEM((nz, count, width), f32),
                pltpu.VMEM((nz, count, width), f32),
                pltpu.VMEM(labels.shape, jnp.int32),
                dma((nz, 2)),
                dma((nz,)),
                dma((nz, 3)),
                dma((nz,)),
                dma((4,)),
                dma((2 + width // LANES,)),
            ],
            compiler_params=pltpu.CompilerParams(collective_id=0, has_side_effects=True, vmem_limit_bytes=67_000_000),
        )(particles, data_rows.reshape(draws, width), labels)

    placed = (P("dom", "dim"), P("dom", None, "dim"), P("dom", None))
    return jax.shard_map(
        per_device, mesh=mesh, in_specs=placed, out_specs=P(None, "dom", "dim"), check_vma=False
    )
```

```python
import functools

import jax
import jax.numpy as jnp
from jax import lax
from jax.experimental import pallas as pl
from jax.experimental.pallas import tpu as pltpu
from jax.sharding import PartitionSpec as P

NEWTON = 2
BAND = 1
LANES = 128

prior_precision = 0.05
like_weight = 4.0
move_size = 0.5
MESH = pl.DeviceIdType.MESH
f32 = jnp.float32
bf16 = jnp.bfloat16


def halves(v):
    high = v.astype(bf16).astype(f32)
    return jnp.concatenate([high, v - high], axis=0).astype(bf16)


def fold(product):
    rows = product.shape[0] // 2
    return product[:rows] + product[rows:]


def paired(product):
    half = product.shape[1] // 2
    return product[:, :half] + product[:, half:]


def dot(a, b):
    return lax.dot_general(a, b, (((1,), (0,)), ((), ())), preferred_element_type=f32)


def dot_t(a, b):
    return lax.dot_general(a, b, (((1,), (1,)), ((), ())), preferred_element_type=f32)


def total_of(values):
    return jnp.sum(jnp.sum(values, axis=0, keepdims=True), axis=1, keepdims=True)


def steps(
    nd, nz, x_ref, a_ref, y_ref, out_ref,
    rows_all, turned, xbuf, xpieces, place, firsts, seconds,
    signs, x_recv, x_over, a_recv, a_over, send, load,
):
    rows, width = x_ref.shape
    draws = a_ref.shape[0]
    per_row = draws // rows
    chips = nd // 2
    slots = nz * nd
    count = nd * rows
    cols = nd * draws
    blocks = width // LANES
    message = blocks * rows + 2
    scale = 1.0 * BAND * width * nz
    cross = 4.0 / (scale * scale)
    me_dom = lax.axis_index("dom")
    z = lax.axis_index("dim")
    chip, core = me_dom // 2, me_dom % 2
    square = chips == 4 and nz == 4

    if square:
        near = [chip + 1 - 2 * (chip % 2), chip + 2 - 4 * (chip // 2), 3 - chip]
        high = z // 2
        middle = (z + 1) // 2 % 2 == 1
        zs = [3 - 3 * high, 2 - high, z + 1 - 2 * (z % 2)]
    else:
        near = [(chip + m) % chips for m in range(1, chips)]
        zs = [(z + k) % nz for k in range(1, nz)]
    partner = {"dom": me_dom + 1 - 2 * core}
    started = {"x": 0, "a": 0}
    sems = {"x": send.at[0], "a": send.at[1], "m": send.at[1]}

    def on_chip(c):
        return {"dom": c * 2 + core}

    def slot(plane, c, k=None):
        return (plane * 2 + (core if k is None else k)) * chips + c

    def copy(kind, ref, recv, device):
        pltpu.make_async_remote_copy(
            src_ref=ref, dst_ref=ref, send_sem=sems[kind], recv_sem=recv,
            device_id=device, device_id_type=MESH,
        ).start()
        if kind in started:
            started[kind] += 1

    def wait(ref, recv):
        pltpu.make_async_remote_copy(
            src_ref=ref, dst_ref=ref, send_sem=send.at[0], recv_sem=recv, device_id=partner, device_id_type=MESH,
        ).wait_recv()

    def wait_sent(ref, kind, number):
        while number > 0:
            part = ref(min(number, slots))
            pltpu.make_async_remote_copy(
                src_ref=part, dst_ref=part, send_sem=sems[kind], recv_sem=send.at[0],
                device_id=partner, device_id_type=MESH,
            ).wait_send()
            number -= slots

    barrier = pltpu.get_barrier_semaphore()
    greet = [on_chip(c) for c in near] + [{"dim": k} for k in zs] + [partner]
    for device in greet:
        pl.semaphore_signal(barrier, inc=1, device_id=device, device_id_type=MESH)

    here = slot(z, chip)
    loads = [
        pltpu.make_async_copy(
            x_ref.at[:, pl.ds(b * LANES, LANES)], xbuf.at[here, pl.ds(b * rows, rows), :], load.at[2]
        )
        for b in range(blocks)
    ]
    loads.append(pltpu.make_async_copy(a_ref, rows_all.at[here], load.at[0]))
    loads.append(pltpu.make_async_copy(y_ref, signs, load.at[1]))
    for one in loads:
        one.start()
    lane_of = lax.broadcasted_iota(jnp.int32, (rows, draws), 1) // per_row
    row_of = lax.broadcasted_iota(jnp.int32, (rows, draws), 0)
    own_block = lane_of == row_of

    def flat(values):
        return jnp.sum(jnp.where(own_block, values, 0.0), axis=0, keepdims=True)

    tile = lax.broadcasted_iota(jnp.int32, (per_row, draws), 1) % per_row
    tile = (tile == lax.broadcasted_iota(jnp.int32, (per_row, draws), 0)).astype(f32).astype(bf16)
    own_places = xbuf.at[here, pl.ds(0, blocks * rows), :]
    pltpu.make_async_copy(own_places, own_places, load.at[2]).wait()
    for one in loads[blocks:]:
        one.wait()
    labels = flat(dot(signs[...].astype(f32).astype(bf16), tile))
    own_x = jnp.concatenate([xbuf[here, b * rows : (b + 1) * rows, :] for b in range(blocks)], axis=1)
    first = flat(fold(dot_t(halves(own_x), rows_all[here])))
    xbuf[here, blocks * rows : blocks * rows + 2, :] = jnp.concatenate([first, labels], axis=0)
    pl.semaphore_wait(barrier, len(greet))

    def xs(at, number=None):
        return xbuf.at[at if number is None else pl.ds(at, number), pl.ds(0, message), :]

    def send_x(plane, devices, recv):
        for device in devices:
            copy("x", xs(slot(plane, chip)), x_recv.at[recv], device)

    def send_a(plane, devices, role):
        for device in devices:
            copy("a", rows_all.at[slot(plane, chip)], a_recv.at[plane, role], device)

    plane_devices = [on_chip(c) for c in near]
    z_devices = [{"dim": k} for k in zs]
    side, diagonal = (near[:2], near[2]) if square else (near, None)
    corner_first = plane_devices[len(side) :] + plane_devices[: len(side)]
    send_x(z, z_devices, z)
    send_x(z, corner_first, nz)
    if square:
        send_a(z, plane_devices[2:], 2)
    send_a(z, plane_devices[: len(side)], 1)
    send_a(z, z_devices, 0)
    for plane in zs:
        wait(xs(slot(plane, chip)), x_recv.at[plane])
        send_x(plane, corner_first, nz)

    def across(plane, c):
        copy("a", rows_all.at[slot(plane, c)], a_over.at[plane], partner)

    for n, plane in enumerate(zs):
        wait(rows_all.at[slot(plane, chip)], a_recv.at[plane, 0])
        if square and n == 0:
            send_a(plane, plane_devices[2:], 2)
        send_a(plane, plane_devices[: len(side)], 1)
        if square and n == 0:
            from_corner = rows_all.at[slot(z, diagonal)]
            wait(from_corner, a_recv.at[z, 2])
            copy("a", from_corner, a_recv.at[z, 2], z_devices[2])

            @pl.when(middle)
            def _():
                for device in z_devices[:2]:
                    copy("m", from_corner, a_recv.at[z, 2], device)

    wait(xs(0, nz * len(near)), x_recv.at[nz])
    for plane in [z] + zs:
        copy("x", xs(slot(plane, 0), chips), x_over.at[0], partner)
        started["x"] += chips - 1

    across(z, chip)
    wait(rows_all.at[pl.ds(0, len(side))], a_recv.at[z, 1])
    for c in near:
        across(z, c)
    for plane in zs:
        across(plane, chip)
    eye = lax.broadcasted_iota(jnp.int32, (count, count), 1) == lax.broadcasted_iota(jnp.int32, (count, count), 0)
    spread_at = lax.broadcasted_iota(jnp.int32, (count, LANES), 1) // per_row
    def row_sums(values):
        return jnp.sum(values, axis=1, keepdims=True)

    def prepare(logits):
        for k in range(nz):
            xpieces[k] = halves(place[k])
        inner = paired(fold(functools.reduce(jnp.add, [dot_t(xpieces[k], xpieces[k]) for k in range(nz)])))
        diagonal = jnp.where(eye, inner, 0.0)
        distance = row_sums(diagonal) + jnp.sum(diagonal, axis=0, keepdims=True) - 2.0 * inner
        kernel = jnp.exp(distance * (-1.0 / scale))
        prob = 1.0 / (1.0 + jnp.exp(-logits))
        curve = like_weight * prob * (1.0 - prob)
        gap = like_weight * (targets - prob)
        kernel_sq = kernel * kernel
        padded = kernel
        if count < LANES:
            padded = jnp.concatenate([kernel, jnp.zeros((count, LANES - count), f32)], axis=1)
        drive, weight = [], []
        for g in range(nd):
            at = g * rows
            block = padded[:, at // LANES * LANES : at // LANES * LANES + LANES]
            wide = jnp.take_along_axis(block, spread_at + at % LANES, axis=1)
            drive.append(wide * gap[g : g + 1])
            weight.append(wide * wide * curve[g : g + 1])
        pull = (-prior_precision - 2.0 / scale) * kernel + jnp.where(eye, (2.0 / scale) * row_sums(kernel), 0.0)
        drive, weight = jnp.concatenate(drive, axis=1), jnp.concatenate(weight, axis=1)
        return kernel_sq, row_sums(kernel_sq), weight, drive, pull

    def basis(k):
        return rows_all[pl.ds(k * nd, nd)].reshape(cols, width)

    def ahead(parts):
        seen = dot(jnp.concatenate([halves(v) for v in parts], axis=1), turned[...])
        along = functools.reduce(jnp.add, [dot_t(parts[k].astype(bf16), xpieces[k, 0:count]) for k in range(nz)])
        return fold(seen), along

    def own_logits(seen):
        return jnp.concatenate(
            [flat(seen[g * rows : (g + 1) * rows, g * draws : (g + 1) * draws]) for g in range(nd)], axis=0
        )


    def hand_over(n):
        plane = zs[n]
        if square and n == 0:
            wait(rows_all.at[slot(plane, diagonal)], a_recv.at[plane, 2])
            across(plane, diagonal)
        wait(rows_all.at[pl.ds(0, len(side))], a_recv.at[plane, 1])
        for c in side:
            across(plane, c)

    def hand_corners():
        if square:
            for plane in zs[:0:-1]:
                wait(rows_all.at[slot(plane, diagonal)], a_recv.at[plane, 2])
                across(plane, diagonal)

    if len(zs) > 0:
        hand_over(0)
    planes = [z] + zs
    wait(xs(0, nz * chips), x_over.at[0])
    for k in range(nz):
        for b in range(blocks):
            block = xbuf[k * nd : (k + 1) * nd, b * rows : (b + 1) * rows, :].reshape(count, LANES)
            place[k, :, b * LANES : (b + 1) * LANES] = block

    def messages(k, row):
        return jnp.concatenate([xbuf[k * nd + g, row : row + 1, :] for g in range(nd)], axis=0)

    logits = functools.reduce(jnp.add, [messages(k, blocks * rows) for k in range(nz)])
    targets = messages(0, blocks * rows + 1)

    kernel_sq, total_sq, weight, drive, pull = prepare(logits)
    left = halves(drive)
    left_x = halves(jnp.concatenate([pull, pull], axis=1))

    def begin(group):
        on_rows, on_places = [], []
        for plane in group:
            rows_here = basis(plane)
            part = fold(dot(left, rows_here) + dot(left_x, xpieces[plane])) / count
            firsts[plane] = part
            turned[pl.ds(pl.multiple_of(plane * width, width), width), :] = rows_here.T
            on_rows.append(dot_t(halves(part), rows_here))
            on_places.append(dot_t(part.astype(bf16), xpieces[plane, 0:count]))
        return fold(functools.reduce(jnp.add, on_rows)), functools.reduce(jnp.add, on_places)

    def landed(plane):
        wait(rows_all.at[pl.ds(slot(plane, 0, 1 - core), chips)], a_over.at[plane])

    landed(z)
    seen, along = begin([z])
    hand_corners()
    for n in range(1, len(zs)):
        hand_over(n)
    for group in (zs[:1], zs[1:]):
        for plane in group:
            landed(plane)
        if group:
            more_seen, more_along = begin(group)
            seen, along = seen + more_seen, along + more_along
    drift = [firsts[k] for k in range(nz)]

    for t in range(NEWTON):
        last = t + 1 == NEWTON
        if t > 0:
            kernel_sq, total_sq, weight, drive, pull = prepare(logits)
            left = halves(drive)
            left_x = halves(jnp.concatenate([pull, pull], axis=1))
            drift = [fold(dot(left, basis(k)) + dot(left_x, xpieces[k])) / count for k in range(nz)]
            for k in range(nz):
                firsts[k] = drift[k]
            seen, along = ahead(drift)
        shift = own_logits(seen)
        on_x = cross * kernel_sq * (along - row_sums(jnp.where(eye, along, 0.0)))
        on_x = on_x - jnp.where(eye, row_sums(on_x), 0.0)
        left, left_x = halves(weight * seen), on_x.astype(bf16)
        image = [
            (fold(dot(left, basis(k))) + dot(left_x, xpieces[k, 0:count]) + prior_precision * total_sq * drift[k])
            / count
            for k in range(nz)
        ]
        for k in range(nz):
            seconds[k] = image[k]
        seen, along = ahead(image)
        shift_image = own_logits(seen)
        along = along - row_sums(jnp.where(eye, along, 0.0))
        norm = total_of(functools.reduce(jnp.add, [d * d for d in drift]))
        curve_total = total_of(functools.reduce(jnp.add, [d * v for d, v in zip(drift, image)]))
        squares = functools.reduce(jnp.add, [v * v for v in image])
        image_square = total_of(squares)
        bent = total_of(prior_precision * total_sq * row_sums(squares) + cross * row_sums(kernel_sq * along * along))
        bent = (bent + total_of(weight * seen * seen)) / count
        alpha = norm / curve_total
        norm_next = norm - 2.0 * alpha * curve_total + alpha * alpha * image_square
        keep = 1.0 + norm_next / norm
        curve_next = keep * keep * curve_total - 2.0 * keep * alpha * image_square + alpha * alpha * bent
        alpha_next = norm_next / curve_next
        on_drift, on_image = alpha + alpha_next * keep, -alpha_next * alpha
        mine = pl.ds(pl.multiple_of((core * chips + chip) * rows, rows), rows)
        out_ref[t] = on_drift * firsts[z, mine, :] + on_image * seconds[z, mine, :]
        if not last:
            step_drift, step_image = move_size * on_drift, move_size * on_image
            for k in range(nz):
                place[k] = place[k] + step_drift * drift[k] + step_image * image[k]
            logits = logits + step_drift * shift + step_image * shift_image
    wait_sent(lambda number: xs(0, number), "x", started["x"])

    def wait_rows(extra):
        wait_sent(lambda number: rows_all.at[pl.ds(0, number)], "a", started["a"] + extra)

    if square:
        pl.when(middle)(lambda: wait_rows(2))
        pl.when(jnp.logical_not(middle))(lambda: wait_rows(0))
    else:
        wait_rows(0)


def solution(mesh):
    nd, nz = mesh.shape["dom"], mesh.shape["dim"]

    def per_device(particles, data_rows, labels):
        rows, width = particles.shape
        draws = data_rows.shape[0] * data_rows.shape[1]
        count = nd * rows
        dma = pltpu.SemaphoreType.DMA
        return pl.pallas_call(
            functools.partial(steps, nd, nz),
            out_shape=pltpu.VMEM((NEWTON, rows, width), f32),
            in_specs=[pl.BlockSpec(memory_space=pl.ANY)] * 3,
            out_specs=pl.BlockSpec(memory_space=pltpu.VMEM),
            scratch_shapes=[
                pltpu.VMEM((nz * nd, draws, width), bf16),
                pltpu.VMEM((nz * width, nd * draws), bf16),
                pltpu.VMEM((nz * nd, -(-(width // LANES * rows + 2) // 8) * 8, LANES), f32),
                pltpu.VMEM((nz, 2 * count, width), bf16),
                pltpu.VMEM((nz, count, width), f32),
                pltpu.VMEM((nz, count, width), f32),
                pltpu.VMEM((nz, count, width), f32),
                pltpu.VMEM(labels.shape, jnp.int32),
                dma((nz + 1,)),
                dma((1,)),
                dma((nz, 3)),
                dma((nz,)),
                dma((2,)),
                dma((3,)),
            ],
            compiler_params=pltpu.CompilerParams(collective_id=0, has_side_effects=True, vmem_limit_bytes=67_000_000),
        )(particles, data_rows.reshape(draws, width), labels)

    placed = (P("dom", "dim"), P("dom", None, "dim"), P("dom", None))
    return jax.shard_map(
        per_device, mesh=mesh, in_specs=placed, out_specs=P(None, "dom", "dim"), check_vma=False
    )
```

```python
import functools

import jax
import jax.numpy as jnp
from jax import lax
from jax.experimental import pallas as pl
from jax.experimental.pallas import tpu as pltpu
from jax.sharding import PartitionSpec as P

NEWTON = 2
BAND = 1
LANES = 128

prior_precision = 0.05
like_weight = 4.0
move_size = 0.5
MESH = pl.DeviceIdType.MESH
f32 = jnp.float32
bf16 = jnp.bfloat16


def halves(v):
    high = v.astype(bf16).astype(f32)
    return jnp.concatenate([high, v - high], axis=0).astype(bf16)


def fold(product):
    rows = product.shape[0] // 2
    return product[:rows] + product[rows:]


def paired(product):
    half = product.shape[1] // 2
    return product[:, :half] + product[:, half:]


def dot(a, b):
    return lax.dot_general(a, b, (((1,), (0,)), ((), ())), preferred_element_type=f32)


def dot_t(a, b):
    return lax.dot_general(a, b, (((1,), (1,)), ((), ())), preferred_element_type=f32)


def total_of(values):
    return jnp.sum(jnp.sum(values, axis=0, keepdims=True), axis=1, keepdims=True)


def steps(
    nd, nz, x_ref, a_ref, y_ref, out_ref,
    rows_all, turned, xbuf, xpieces, place, firsts, seconds,
    signs, x_recv, x_over, a_recv, a_over, send, load,
):
    rows, width = x_ref.shape
    draws = a_ref.shape[0]
    per_row = draws // rows
    chips = nd // 2
    slots = nz * nd
    count = nd * rows
    cols = nd * draws
    blocks = width // LANES
    message = blocks * rows + 2
    scale = 1.0 * BAND * width * nz
    cross = 4.0 / (scale * scale)
    me_dom = lax.axis_index("dom")
    z = lax.axis_index("dim")
    chip, core = me_dom // 2, me_dom % 2
    square = chips == 4 and nz == 4

    if square:
        near = [chip + 1 - 2 * (chip % 2), chip + 2 - 4 * (chip // 2), 3 - chip]
        high = z // 2
        middle = (z + 1) // 2 % 2 == 1
        zs = [3 - 3 * high, 2 - high, z + 1 - 2 * (z % 2)]
    else:
        near = [(chip + m) % chips for m in range(1, chips)]
        zs = [(z + k) % nz for k in range(1, nz)]
    partner = {"dom": me_dom + 1 - 2 * core}
    started = {"x": 0, "a": 0}
    sems = {"x": send.at[0], "a": send.at[1], "m": send.at[1]}

    def on_chip(c):
        return {"dom": c * 2 + core}

    def slot(plane, c, k=None):
        return (plane * 2 + (core if k is None else k)) * chips + c

    def copy(kind, ref, recv, device):
        pltpu.make_async_remote_copy(
            src_ref=ref, dst_ref=ref, send_sem=sems[kind], recv_sem=recv,
            device_id=device, device_id_type=MESH,
        ).start()
        if kind in started:
            started[kind] += 1

    def wait(ref, recv):
        pltpu.make_async_remote_copy(
            src_ref=ref, dst_ref=ref, send_sem=send.at[0], recv_sem=recv, device_id=partner, device_id_type=MESH,
        ).wait_recv()

    def wait_sent(ref, kind, number):
        while number > 0:
            part = ref(min(number, slots))
            pltpu.make_async_remote_copy(
                src_ref=part, dst_ref=part, send_sem=sems[kind], recv_sem=send.at[0],
                device_id=partner, device_id_type=MESH,
            ).wait_send()
            number -= slots

    barrier = pltpu.get_barrier_semaphore()
    greet = [on_chip(c) for c in near] + [{"dim": k} for k in zs] + [partner]
    for device in greet:
        pl.semaphore_signal(barrier, inc=1, device_id=device, device_id_type=MESH)

    here = slot(z, chip)
    loads = [
        pltpu.make_async_copy(
            x_ref.at[:, pl.ds(b * LANES, LANES)], xbuf.at[here, pl.ds(b * rows, rows), :], load.at[2]
        )
        for b in range(blocks)
    ]
    loads.append(pltpu.make_async_copy(a_ref, rows_all.at[here], load.at[0]))
    loads.append(pltpu.make_async_copy(y_ref, signs, load.at[1]))
    for one in loads:
        one.start()
    lane_of = lax.broadcasted_iota(jnp.int32, (rows, draws), 1) // per_row
    row_of = lax.broadcasted_iota(jnp.int32, (rows, draws), 0)
    own_block = lane_of == row_of

    def flat(values):
        return jnp.sum(jnp.where(own_block, values, 0.0), axis=0, keepdims=True)

    tile = lax.broadcasted_iota(jnp.int32, (per_row, draws), 1) % per_row
    tile = (tile == lax.broadcasted_iota(jnp.int32, (per_row, draws), 0)).astype(f32).astype(bf16)
    own_places = xbuf.at[here, pl.ds(0, blocks * rows), :]
    pltpu.make_async_copy(own_places, own_places, load.at[2]).wait()
    for one in loads[blocks:]:
        one.wait()
    labels = flat(dot(signs[...].astype(f32).astype(bf16), tile))
    own_x = jnp.concatenate([xbuf[here, b * rows : (b + 1) * rows, :] for b in range(blocks)], axis=1)
    first = flat(fold(dot_t(halves(own_x), rows_all[here])))
    xbuf[here, blocks * rows : blocks * rows + 2, :] = jnp.concatenate([first, labels], axis=0)
    pl.semaphore_wait(barrier, len(greet))

    def xs(at, number=None):
        return xbuf.at[at if number is None else pl.ds(at, number), pl.ds(0, message), :]

    def send_x(plane, devices, recv):
        for device in devices:
            copy("x", xs(slot(plane, chip)), x_recv.at[recv], device)

    def send_a(plane, devices, role):
        for device in devices:
            copy("a", rows_all.at[slot(plane, chip)], a_recv.at[plane, role], device)

    plane_devices = [on_chip(c) for c in near]
    z_devices = [{"dim": k} for k in zs]
    side, diagonal = (near[:2], near[2]) if square else (near, None)
    corner_first = plane_devices[len(side) :] + plane_devices[: len(side)]
    send_x(z, z_devices, z)
    send_x(z, corner_first, nz)
    if square:
        send_a(z, plane_devices[2:], 2)
    send_a(z, plane_devices[: len(side)], 1)
    send_a(z, z_devices, 0)
    for plane in zs:
        wait(xs(slot(plane, chip)), x_recv.at[plane])
        send_x(plane, corner_first, nz)

    def across(plane, c):
        copy("a", rows_all.at[slot(plane, c)], a_over.at[plane], partner)

    for n, plane in enumerate(zs):
        wait(rows_all.at[slot(plane, chip)], a_recv.at[plane, 0])
        if square and n == 0:
            send_a(plane, plane_devices[2:], 2)
        send_a(plane, plane_devices[: len(side)], 1)
        if square and n == 0:
            from_corner = rows_all.at[slot(z, diagonal)]
            wait(from_corner, a_recv.at[z, 2])
            copy("a", from_corner, a_recv.at[z, 2], z_devices[2])

            @pl.when(middle)
            def _():
                for device in z_devices[:2]:
                    copy("m", from_corner, a_recv.at[z, 2], device)

    wait(xs(0, nz * len(near)), x_recv.at[nz])
    for plane in [z] + zs:
        copy("x", xs(slot(plane, 0), chips), x_over.at[0], partner)
        started["x"] += chips - 1

    across(z, chip)
    wait(rows_all.at[pl.ds(0, len(side))], a_recv.at[z, 1])
    for c in near:
        across(z, c)
    for plane in zs:
        across(plane, chip)
    eye = lax.broadcasted_iota(jnp.int32, (count, count), 1) == lax.broadcasted_iota(jnp.int32, (count, count), 0)
    spread_at = lax.broadcasted_iota(jnp.int32, (count, LANES), 1) // per_row
    def row_sums(values):
        return jnp.sum(values, axis=1, keepdims=True)

    def prepare(logits):
        for k in range(nz):
            xpieces[k] = halves(place[k])
        inner = paired(fold(functools.reduce(jnp.add, [dot_t(xpieces[k], xpieces[k]) for k in range(nz)])))
        diagonal = jnp.where(eye, inner, 0.0)
        distance = row_sums(diagonal) + jnp.sum(diagonal, axis=0, keepdims=True) - 2.0 * inner
        kernel = jnp.exp(distance * (-1.0 / scale))
        prob = 1.0 / (1.0 + jnp.exp(-logits))
        curve = like_weight * prob * (1.0 - prob)
        gap = like_weight * (targets - prob)
        kernel_sq = kernel * kernel
        padded = kernel
        if count < LANES:
            padded = jnp.concatenate([kernel, jnp.zeros((count, LANES - count), f32)], axis=1)
        drive, weight = [], []
        for g in range(nd):
            at = g * rows
            block = padded[:, at // LANES * LANES : at // LANES * LANES + LANES]
            wide = jnp.take_along_axis(block, spread_at + at % LANES, axis=1)
            drive.append(wide * gap[g : g + 1])
            weight.append(wide * wide * curve[g : g + 1])
        pull = (-prior_precision - 2.0 / scale) * kernel + jnp.where(eye, (2.0 / scale) * row_sums(kernel), 0.0)
        drive, weight = jnp.concatenate(drive, axis=1), jnp.concatenate(weight, axis=1)
        return kernel, gap, kernel_sq, row_sums(kernel_sq), weight, drive, pull

    def basis(k):
        return rows_all[pl.ds(k * nd, nd)].reshape(cols, width)

    def ahead(parts):
        seen = dot(jnp.concatenate([halves(v) for v in parts], axis=1), turned[...])
        along = functools.reduce(jnp.add, [dot_t(parts[k].astype(bf16), xpieces[k, 0:count]) for k in range(nz)])
        return fold(seen), along

    def own_rows(values):
        lines = []
        for g in range(nd):
            line = [jnp.zeros((rows, g * draws), f32)] if g > 0 else []
            line.append(jnp.where(own_block, values[g : g + 1], 0.0))
            if g + 1 < nd:
                line.append(jnp.zeros((rows, cols - (g + 1) * draws), f32))
            lines.append(jnp.concatenate(line, axis=1))
        return jnp.concatenate(lines, axis=0)

    def own_logits(seen):
        return jnp.concatenate(
            [flat(seen[g * rows : (g + 1) * rows, g * draws : (g + 1) * draws]) for g in range(nd)], axis=0
        )


    def hand_over(n):
        plane = zs[n]
        if square and n == 0:
            wait(rows_all.at[slot(plane, diagonal)], a_recv.at[plane, 2])
            across(plane, diagonal)
        wait(rows_all.at[pl.ds(0, len(side))], a_recv.at[plane, 1])
        for c in side:
            across(plane, c)

    def hand_corners():
        if square:
            for plane in zs[:0:-1]:
                wait(rows_all.at[slot(plane, diagonal)], a_recv.at[plane, 2])
                across(plane, diagonal)

    if len(zs) > 0:
        hand_over(0)
    planes = [z] + zs
    wait(xs(0, nz * chips), x_over.at[0])
    for k in range(nz):
        for b in range(blocks):
            block = xbuf[k * nd : (k + 1) * nd, b * rows : (b + 1) * rows, :].reshape(count, LANES)
            place[k, :, b * LANES : (b + 1) * LANES] = block

    def messages(k, row):
        return jnp.concatenate([xbuf[k * nd + g, row : row + 1, :] for g in range(nd)], axis=0)

    logits = functools.reduce(jnp.add, [messages(k, blocks * rows) for k in range(nz)])
    targets = messages(0, blocks * rows + 1)

    _, _, kernel_sq, total_sq, weight, drive, pull = prepare(logits)
    left = halves(drive)
    left_x = halves(jnp.concatenate([pull, pull], axis=1))

    def begin(group):
        on_rows, on_places = [], []
        for plane in group:
            rows_here = basis(plane)
            part = fold(dot(left, rows_here) + dot(left_x, xpieces[plane])) / count
            firsts[plane] = part
            turned[pl.ds(pl.multiple_of(plane * width, width), width), :] = rows_here.T
            on_rows.append(dot_t(halves(part), rows_here))
            on_places.append(dot_t(part.astype(bf16), xpieces[plane, 0:count]))
        return fold(functools.reduce(jnp.add, on_rows)), functools.reduce(jnp.add, on_places)

    def landed(plane):
        wait(rows_all.at[pl.ds(slot(plane, 0, 1 - core), chips)], a_over.at[plane])

    landed(z)
    seen, along = begin([z])
    hand_corners()
    for n in range(1, len(zs)):
        hand_over(n)
    for group in (zs[:1], zs[1:]):
        for plane in group:
            landed(plane)
        if group:
            more_seen, more_along = begin(group)
            seen, along = seen + more_seen, along + more_along
    drift = [firsts[k] for k in range(nz)]

    for t in range(NEWTON):
        last = t + 1 == NEWTON
        if t > 0:
            kernel, gap, kernel_sq, total_sq, weight, _, _ = prepare(logits)
            left = halves(own_rows(gap))
            left_x = halves(jnp.concatenate([kernel, kernel], axis=1))
            inward, outward = prior_precision + 2.0 / scale, (2.0 / scale) * row_sums(kernel)
            pulled = [halves(fold(dot(left, basis(k))) - inward * place[k]) for k in range(nz)]
            drift = [(fold(dot(left_x, pulled[k])) + outward * place[k]) / count for k in range(nz)]
            for k in range(nz):
                firsts[k] = drift[k]
            seen, along = ahead(drift)
        shift = own_logits(seen)
        on_x = cross * kernel_sq * (along - row_sums(jnp.where(eye, along, 0.0)))
        on_x = on_x - jnp.where(eye, row_sums(on_x), 0.0)
        left, left_x = halves(weight * seen), on_x.astype(bf16)
        image = [
            (fold(dot(left, basis(k))) + dot(left_x, xpieces[k, 0:count]) + prior_precision * total_sq * drift[k])
            / count
            for k in range(nz)
        ]
        for k in range(nz):
            seconds[k] = image[k]
        seen, along = ahead(image)
        shift_image = own_logits(seen)
        along = along - row_sums(jnp.where(eye, along, 0.0))
        norm = total_of(functools.reduce(jnp.add, [d * d for d in drift]))
        curve_total = total_of(functools.reduce(jnp.add, [d * v for d, v in zip(drift, image)]))
        squares = functools.reduce(jnp.add, [v * v for v in image])
        image_square = total_of(squares)
        bent = total_of(prior_precision * total_sq * row_sums(squares) + cross * row_sums(kernel_sq * along * along))
        bent = (bent + total_of(weight * seen * seen)) / count
        alpha = norm / curve_total
        norm_next = norm - 2.0 * alpha * curve_total + alpha * alpha * image_square
        keep = 1.0 + norm_next / norm
        curve_next = keep * keep * curve_total - 2.0 * keep * alpha * image_square + alpha * alpha * bent
        alpha_next = norm_next / curve_next
        on_drift, on_image = alpha + alpha_next * keep, -alpha_next * alpha
        mine = pl.ds(pl.multiple_of((core * chips + chip) * rows, rows), rows)
        out_ref[t] = on_drift * firsts[z, mine, :] + on_image * seconds[z, mine, :]
        if not last:
            step_drift, step_image = move_size * on_drift, move_size * on_image
            for k in range(nz):
                place[k] = place[k] + step_drift * drift[k] + step_image * image[k]
            logits = logits + step_drift * shift + step_image * shift_image
    wait_sent(lambda number: xs(0, number), "x", started["x"])

    def wait_rows(extra):
        wait_sent(lambda number: rows_all.at[pl.ds(0, number)], "a", started["a"] + extra)

    if square:
        pl.when(middle)(lambda: wait_rows(2))
        pl.when(jnp.logical_not(middle))(lambda: wait_rows(0))
    else:
        wait_rows(0)


def solution(mesh):
    nd, nz = mesh.shape["dom"], mesh.shape["dim"]

    def per_device(particles, data_rows, labels):
        rows, width = particles.shape
        draws = data_rows.shape[0] * data_rows.shape[1]
        count = nd * rows
        dma = pltpu.SemaphoreType.DMA
        return pl.pallas_call(
            functools.partial(steps, nd, nz),
            out_shape=pltpu.VMEM((NEWTON, rows, width), f32),
            in_specs=[pl.BlockSpec(memory_space=pl.ANY)] * 3,
            out_specs=pl.BlockSpec(memory_space=pltpu.VMEM),
            scratch_shapes=[
                pltpu.VMEM((nz * nd, draws, width), bf16),
                pltpu.VMEM((nz * width, nd * draws), bf16),
                pltpu.VMEM((nz * nd, -(-(width // LANES * rows + 2) // 8) * 8, LANES), f32),
                pltpu.VMEM((nz, 2 * count, width), bf16),
                pltpu.VMEM((nz, count, width), f32),
                pltpu.VMEM((nz, count, width), f32),
                pltpu.VMEM((nz, count, width), f32),
                pltpu.VMEM(labels.shape, jnp.int32),
                dma((nz + 1,)),
                dma((1,)),
                dma((nz, 3)),
                dma((nz,)),
                dma((2,)),
                dma((3,)),
            ],
            compiler_params=pltpu.CompilerParams(collective_id=0, has_side_effects=True, vmem_limit_bytes=67_000_000),
        )(particles, data_rows.reshape(draws, width), labels)

    placed = (P("dom", "dim"), P("dom", None, "dim"), P("dom", None))
    return jax.shard_map(
        per_device, mesh=mesh, in_specs=placed, out_specs=P(None, "dom", "dim"), check_vma=False
    )
```

```python
import functools

import jax
import jax.numpy as jnp
from jax import lax
from jax.experimental import pallas as pl
from jax.experimental.pallas import tpu as pltpu
from jax.sharding import PartitionSpec as P

NEWTON = 2
BAND = 1
LANES = 128

prior_precision = 0.05
like_weight = 4.0
move_size = 0.5
MESH = pl.DeviceIdType.MESH
f32 = jnp.float32
bf16 = jnp.bfloat16


def halves(v):
    high = v.astype(bf16).astype(f32)
    return jnp.concatenate([high, v - high], axis=0).astype(bf16)


def fold(product):
    rows = product.shape[0] // 2
    return product[:rows] + product[rows:]


def paired(product):
    half = product.shape[1] // 2
    return product[:, :half] + product[:, half:]


def dot(a, b):
    return lax.dot_general(a, b, (((1,), (0,)), ((), ())), preferred_element_type=f32)


def dot_t(a, b):
    return lax.dot_general(a, b, (((1,), (1,)), ((), ())), preferred_element_type=f32)


def total_of(values):
    return jnp.sum(jnp.sum(values, axis=0, keepdims=True), axis=1, keepdims=True)


def steps(
    nd, nz, x_ref, a_ref, y_ref, out_ref,
    rows_all, turned, xbuf, xpieces, place, firsts, seconds,
    signs, x_recv, x_over, a_recv, a_over, send, load,
):
    rows, width = x_ref.shape
    draws = a_ref.shape[0]
    per_row = draws // rows
    chips = nd // 2
    slots = nz * nd
    count = nd * rows
    cols = nd * draws
    blocks = width // LANES
    message = blocks * rows + 2
    scale = 1.0 * BAND * width * nz
    cross = 4.0 / (scale * scale)
    me_dom = lax.axis_index("dom")
    z = lax.axis_index("dim")
    chip, core = me_dom // 2, me_dom % 2
    square = chips == 4 and nz == 4

    if square:
        near = [chip + 1 - 2 * (chip % 2), chip + 2 - 4 * (chip // 2), 3 - chip]
        high = z // 2
        middle = (z + 1) // 2 % 2 == 1
        zs = [3 - 3 * high, 2 - high, z + 1 - 2 * (z % 2)]
    else:
        near = [(chip + m) % chips for m in range(1, chips)]
        zs = [(z + k) % nz for k in range(1, nz)]
    partner = {"dom": me_dom + 1 - 2 * core}
    started = {"x": 0, "a": 0}
    sems = {"x": send.at[0], "a": send.at[1], "m": send.at[1]}

    def on_chip(c):
        return {"dom": c * 2 + core}

    def slot(plane, c, k=None):
        return (plane * 2 + (core if k is None else k)) * chips + c

    def copy(kind, ref, recv, device):
        pltpu.make_async_remote_copy(
            src_ref=ref, dst_ref=ref, send_sem=sems[kind], recv_sem=recv,
            device_id=device, device_id_type=MESH,
        ).start()
        if kind in started:
            started[kind] += 1

    def wait(ref, recv):
        pltpu.make_async_remote_copy(
            src_ref=ref, dst_ref=ref, send_sem=send.at[0], recv_sem=recv, device_id=partner, device_id_type=MESH,
        ).wait_recv()

    def wait_sent(ref, kind, number):
        while number > 0:
            part = ref(min(number, slots))
            pltpu.make_async_remote_copy(
                src_ref=part, dst_ref=part, send_sem=sems[kind], recv_sem=send.at[0],
                device_id=partner, device_id_type=MESH,
            ).wait_send()
            number -= slots

    barrier = pltpu.get_barrier_semaphore()
    greet = [on_chip(c) for c in near] + [{"dim": k} for k in zs] + [partner]
    for device in greet:
        pl.semaphore_signal(barrier, inc=1, device_id=device, device_id_type=MESH)

    here = slot(z, chip)
    loads = [
        pltpu.make_async_copy(
            x_ref.at[:, pl.ds(b * LANES, LANES)], xbuf.at[here, pl.ds(b * rows, rows), :], load.at[2]
        )
        for b in range(blocks)
    ]
    loads.append(pltpu.make_async_copy(a_ref, rows_all.at[here], load.at[0]))
    loads.append(pltpu.make_async_copy(y_ref, signs, load.at[1]))
    for one in loads:
        one.start()
    lane_of = lax.broadcasted_iota(jnp.int32, (rows, draws), 1) // per_row
    row_of = lax.broadcasted_iota(jnp.int32, (rows, draws), 0)
    own_block = lane_of == row_of

    def flat(values):
        return jnp.sum(jnp.where(own_block, values, 0.0), axis=0, keepdims=True)

    tile = lax.broadcasted_iota(jnp.int32, (per_row, draws), 1) % per_row
    tile = (tile == lax.broadcasted_iota(jnp.int32, (per_row, draws), 0)).astype(f32).astype(bf16)
    own_places = xbuf.at[here, pl.ds(0, blocks * rows), :]
    pltpu.make_async_copy(own_places, own_places, load.at[2]).wait()
    for one in loads[blocks:]:
        one.wait()
    labels = flat(dot(signs[...].astype(f32).astype(bf16), tile))
    own_x = jnp.concatenate([xbuf[here, b * rows : (b + 1) * rows, :] for b in range(blocks)], axis=1)
    first = flat(fold(dot_t(halves(own_x), rows_all[here])))
    xbuf[here, blocks * rows : blocks * rows + 2, :] = jnp.concatenate([first, labels], axis=0)
    pl.semaphore_wait(barrier, len(greet))

    def xs(at, number=None):
        return xbuf.at[at if number is None else pl.ds(at, number), pl.ds(0, message), :]

    def send_x(plane, devices, recv):
        for device in devices:
            copy("x", xs(slot(plane, chip)), x_recv.at[recv], device)

    def send_a(plane, devices, role):
        for device in devices:
            copy("a", rows_all.at[slot(plane, chip)], a_recv.at[plane, role], device)

    plane_devices = [on_chip(c) for c in near]
    z_devices = [{"dim": k} for k in zs]
    side, diagonal = (near[:2], near[2]) if square else (near, None)
    corner_first = plane_devices[len(side) :] + plane_devices[: len(side)]
    send_x(z, z_devices, z)
    send_x(z, corner_first, nz)
    if square:
        send_a(z, plane_devices[2:], 2)
    send_a(z, plane_devices[: len(side)], 1)
    send_a(z, z_devices, 0)
    for plane in zs:
        wait(xs(slot(plane, chip)), x_recv.at[plane])
        send_x(plane, corner_first, nz)

    def across(plane, c):
        copy("a", rows_all.at[slot(plane, c)], a_over.at[plane], partner)

    for n, plane in enumerate(zs):
        wait(rows_all.at[slot(plane, chip)], a_recv.at[plane, 0])
        if square and n == 0:
            send_a(plane, plane_devices[2:], 2)
        send_a(plane, plane_devices[: len(side)], 1)
        if square and n == 0:
            from_corner = rows_all.at[slot(z, diagonal)]
            wait(from_corner, a_recv.at[z, 2])
            copy("a", from_corner, a_recv.at[z, 2], z_devices[2])

            @pl.when(middle)
            def _():
                for device in z_devices[:2]:
                    copy("m", from_corner, a_recv.at[z, 2], device)

    wait(xs(0, nz * len(near)), x_recv.at[nz])
    for plane in [z] + zs:
        copy("x", xs(slot(plane, 0), chips), x_over.at[0], partner)
        started["x"] += chips - 1

    across(z, chip)
    wait(rows_all.at[pl.ds(0, len(side))], a_recv.at[z, 1])
    for c in near:
        across(z, c)
    for plane in zs:
        across(plane, chip)
    eye = lax.broadcasted_iota(jnp.int32, (count, count), 1) == lax.broadcasted_iota(jnp.int32, (count, count), 0)
    spread_at = lax.broadcasted_iota(jnp.int32, (count, LANES), 1) // per_row
    def row_sums(values):
        return jnp.sum(values, axis=1, keepdims=True)

    def prepare(logits):
        for k in range(nz):
            xpieces[k] = halves(place[k])
        inner = paired(fold(functools.reduce(jnp.add, [dot_t(xpieces[k], xpieces[k]) for k in range(nz)])))
        diagonal = jnp.where(eye, inner, 0.0)
        distance = row_sums(diagonal) + jnp.sum(diagonal, axis=0, keepdims=True) - 2.0 * inner
        kernel = jnp.exp(distance * (-1.0 / scale))
        prob = 1.0 / (1.0 + jnp.exp(-logits))
        curve = like_weight * prob * (1.0 - prob)
        gap = like_weight * (targets - prob)
        kernel_sq = kernel * kernel
        padded = kernel
        if count < LANES:
            padded = jnp.concatenate([kernel, jnp.zeros((count, LANES - count), f32)], axis=1)
        drive, weight = [], []
        for g in range(nd):
            at = g * rows
            block = padded[:, at // LANES * LANES : at // LANES * LANES + LANES]
            wide = jnp.take_along_axis(block, spread_at + at % LANES, axis=1)
            drive.append(wide * gap[g : g + 1])
            weight.append(wide * wide * curve[g : g + 1])
        pull = (-prior_precision - 2.0 / scale) * kernel + jnp.where(eye, (2.0 / scale) * row_sums(kernel), 0.0)
        drive, weight = jnp.concatenate(drive, axis=1), jnp.concatenate(weight, axis=1)
        return kernel, gap, kernel_sq, row_sums(kernel_sq), weight, drive, pull

    def basis(k):
        return rows_all[pl.ds(k * nd, nd)].reshape(cols, width)

    def ahead(parts, exact=True):
        pieces = [halves(v) if exact else v.astype(bf16) for v in parts]
        seen = dot(jnp.concatenate(pieces, axis=1), turned[...])
        along = functools.reduce(jnp.add, [dot_t(parts[k].astype(bf16), xpieces[k, 0:count]) for k in range(nz)])
        return fold(seen) if exact else seen, along

    def own_rows(values):
        lines = []
        for g in range(nd):
            line = [jnp.zeros((rows, g * draws), f32)] if g > 0 else []
            line.append(jnp.where(own_block, values[g : g + 1], 0.0))
            if g + 1 < nd:
                line.append(jnp.zeros((rows, cols - (g + 1) * draws), f32))
            lines.append(jnp.concatenate(line, axis=1))
        return jnp.concatenate(lines, axis=0)

    def own_logits(seen):
        return jnp.concatenate(
            [flat(seen[g * rows : (g + 1) * rows, g * draws : (g + 1) * draws]) for g in range(nd)], axis=0
        )


    def hand_over(n):
        plane = zs[n]
        if square and n == 0:
            wait(rows_all.at[slot(plane, diagonal)], a_recv.at[plane, 2])
            across(plane, diagonal)
        wait(rows_all.at[pl.ds(0, len(side))], a_recv.at[plane, 1])
        for c in side:
            across(plane, c)

    def hand_corners():
        if square:
            for plane in zs[:0:-1]:
                wait(rows_all.at[slot(plane, diagonal)], a_recv.at[plane, 2])
                across(plane, diagonal)

    if len(zs) > 0:
        hand_over(0)
    planes = [z] + zs
    wait(xs(0, nz * chips), x_over.at[0])
    for k in range(nz):
        for b in range(blocks):
            block = xbuf[k * nd : (k + 1) * nd, b * rows : (b + 1) * rows, :].reshape(count, LANES)
            place[k, :, b * LANES : (b + 1) * LANES] = block

    def messages(k, row):
        return jnp.concatenate([xbuf[k * nd + g, row : row + 1, :] for g in range(nd)], axis=0)

    logits = functools.reduce(jnp.add, [messages(k, blocks * rows) for k in range(nz)])
    targets = messages(0, blocks * rows + 1)

    _, _, kernel_sq, total_sq, weight, drive, pull = prepare(logits)
    left = halves(drive)
    left_x = halves(jnp.concatenate([pull, pull], axis=1))

    def begin(group):
        on_rows, on_places = [], []
        for plane in group:
            rows_here = basis(plane)
            part = fold(dot(left, rows_here) + dot(left_x, xpieces[plane])) / count
            firsts[plane] = part
            turned[pl.ds(pl.multiple_of(plane * width, width), width), :] = rows_here.T
            on_rows.append(dot_t(halves(part), rows_here))
            on_places.append(dot_t(part.astype(bf16), xpieces[plane, 0:count]))
        return fold(functools.reduce(jnp.add, on_rows)), functools.reduce(jnp.add, on_places)

    def landed(plane):
        wait(rows_all.at[pl.ds(slot(plane, 0, 1 - core), chips)], a_over.at[plane])

    landed(z)
    seen, along = begin([z])
    hand_corners()
    for n in range(1, len(zs)):
        hand_over(n)
    for group in (zs[:1], zs[1:]):
        for plane in group:
            landed(plane)
        if group:
            more_seen, more_along = begin(group)
            seen, along = seen + more_seen, along + more_along
    drift = [firsts[k] for k in range(nz)]

    for t in range(NEWTON):
        last = t + 1 == NEWTON
        if t > 0:
            kernel, gap, kernel_sq, total_sq, weight, _, _ = prepare(logits)
            left = halves(own_rows(gap))
            left_x = halves(jnp.concatenate([kernel, kernel], axis=1))
            inward, outward = prior_precision + 2.0 / scale, (2.0 / scale) * row_sums(kernel)
            pulled = [halves(fold(dot(left, basis(k))) - inward * place[k]) for k in range(nz)]
            drift = [(fold(dot(left_x, pulled[k])) + outward * place[k]) / count for k in range(nz)]
            for k in range(nz):
                firsts[k] = drift[k]
            seen, along = ahead(drift)
        shift = own_logits(seen)
        on_x = cross * kernel_sq * (along - row_sums(jnp.where(eye, along, 0.0)))
        on_x = on_x - jnp.where(eye, row_sums(on_x), 0.0)
        left, left_x = halves(weight * seen), on_x.astype(bf16)
        image = [
            (fold(dot(left, basis(k))) + dot(left_x, xpieces[k, 0:count]) + prior_precision * total_sq * drift[k])
            / count
            for k in range(nz)
        ]
        for k in range(nz):
            seconds[k] = image[k]
        seen, along = ahead(image, not last)
        shift_image = own_logits(seen)
        along = along - row_sums(jnp.where(eye, along, 0.0))
        norm = total_of(functools.reduce(jnp.add, [d * d for d in drift]))
        curve_total = total_of(functools.reduce(jnp.add, [d * v for d, v in zip(drift, image)]))
        squares = functools.reduce(jnp.add, [v * v for v in image])
        image_square = total_of(squares)
        bent = total_of(prior_precision * total_sq * row_sums(squares) + cross * row_sums(kernel_sq * along * along))
        bent = (bent + total_of(weight * seen * seen)) / count
        alpha = norm / curve_total
        norm_next = norm - 2.0 * alpha * curve_total + alpha * alpha * image_square
        keep = 1.0 + norm_next / norm
        curve_next = keep * keep * curve_total - 2.0 * keep * alpha * image_square + alpha * alpha * bent
        alpha_next = norm_next / curve_next
        on_drift, on_image = alpha + alpha_next * keep, -alpha_next * alpha
        mine = pl.ds(pl.multiple_of((core * chips + chip) * rows, rows), rows)
        out_ref[t] = on_drift * firsts[z, mine, :] + on_image * seconds[z, mine, :]
        if not last:
            step_drift, step_image = move_size * on_drift, move_size * on_image
            for k in range(nz):
                place[k] = place[k] + step_drift * drift[k] + step_image * image[k]
            logits = logits + step_drift * shift + step_image * shift_image
    wait_sent(lambda number: xs(0, number), "x", started["x"])

    def wait_rows(extra):
        wait_sent(lambda number: rows_all.at[pl.ds(0, number)], "a", started["a"] + extra)

    if square:
        pl.when(middle)(lambda: wait_rows(2))
        pl.when(jnp.logical_not(middle))(lambda: wait_rows(0))
    else:
        wait_rows(0)


def solution(mesh):
    nd, nz = mesh.shape["dom"], mesh.shape["dim"]

    def per_device(particles, data_rows, labels):
        rows, width = particles.shape
        draws = data_rows.shape[0] * data_rows.shape[1]
        count = nd * rows
        dma = pltpu.SemaphoreType.DMA
        return pl.pallas_call(
            functools.partial(steps, nd, nz),
            out_shape=pltpu.VMEM((NEWTON, rows, width), f32),
            in_specs=[pl.BlockSpec(memory_space=pl.ANY)] * 3,
            out_specs=pl.BlockSpec(memory_space=pltpu.VMEM),
            scratch_shapes=[
                pltpu.VMEM((nz * nd, draws, width), bf16),
                pltpu.VMEM((nz * width, nd * draws), bf16),
                pltpu.VMEM((nz * nd, -(-(width // LANES * rows + 2) // 8) * 8, LANES), f32),
                pltpu.VMEM((nz, 2 * count, width), bf16),
                pltpu.VMEM((nz, count, width), f32),
                pltpu.VMEM((nz, count, width), f32),
                pltpu.VMEM((nz, count, width), f32),
                pltpu.VMEM(labels.shape, jnp.int32),
                dma((nz + 1,)),
                dma((1,)),
                dma((nz, 3)),
                dma((nz,)),
                dma((2,)),
                dma((3,)),
            ],
            compiler_params=pltpu.CompilerParams(collective_id=0, has_side_effects=True, vmem_limit_bytes=67_000_000),
        )(particles, data_rows.reshape(draws, width), labels)

    placed = (P("dom", "dim"), P("dom", None, "dim"), P("dom", None))
    return jax.shard_map(
        per_device, mesh=mesh, in_specs=placed, out_specs=P(None, "dom", "dim"), check_vma=False
    )
```
